32 devices in a mesh: member: 4 (over y, x), grid: 8 (over z, core).
Axes of the slice: x: 2, y: 2, z: 4, core: 2. Of those that a mesh axis runs over, the one named last changes fastest.
Arguments:
- prior_ensemble: bfloat16 [40, 48, 32768], P('member', None, 'grid'), may hold values from -6 to 6
- domain_site_mapping: int32 [8, 4, 1024], P(None, None, 'grid'), may hold values from 0 to 4095, as said below
- neighbour_triples: int32 [8, 3, 4096], P('grid', None, 'member'), may hold values from 0 to 159
- stencil_factors: float32 [8, 3, 4096], P('grid', None, 'member'), may hold values from 0.1 to 1
- sparse_node_transforms: float32 [1600, 1024], P(None, 'grid'), may hold values from -0.4 to 1.8
Outputs:
- analysis: bfloat16 [40, 48, 32768], P('member', None, 'grid')
The draws below stay inside these ranges and needn't reach their ends.
Inputs may be any that keep to these rules, and one draw needn't show every extreme that they name: For every model patch h, the entries domain_site_mapping[:, :, h * 128 : (h + 1) * 128] hold every number from 0 to 4095 exactly once.
All inputs are finite; a program needn't handle non-finite values.
Results may differ from the reference program's by a relative error of at most 0.0076.
Values may be sent and summed in bfloat16 or wider, within the bound.
A program may use at most 128 MiB of HBM per device.

```python
import math
import jax
import jax.numpy as jnp
from jax import lax

ENSEMBLE_SIZE = 40
STATE_QUANTITIES = 48
CELLS_DEV = 4096
COARSE_DEV = 128
RIM = 16
PATCHES = 8
GROUPS = 4
COLUMNS = 1024
PER_SOURCE = 128
MESH_SITES = 32768
COARSE = 1024


def draw_domain_site_mapping(key, part):
    subkeys = jax.random.split(jax.random.fold_in(key, 11), PATCHES)
    shuffled = jax.vmap(lambda subkey: jax.random.permutation(subkey, CELLS_DEV))(subkeys)
    shuffled = shuffled.reshape(PATCHES, PATCHES, GROUPS, PER_SOURCE)
    return jnp.transpose(shuffled, (1, 2, 0, 3)).reshape(PATCHES, GROUPS, COLUMNS).astype(jnp.int32)


def draw_sparse_node_transforms(key, part):
    first_key = jax.random.fold_in(key, 21)
    second_key = jax.random.fold_in(key, 22)
    scatter_part = jnp.clip(0.12 * jax.random.normal(first_key, (ENSEMBLE_SIZE, ENSEMBLE_SIZE, COARSE), jnp.float32), -0.4, 0.4)
    diagonal_part = jax.random.uniform(second_key, (ENSEMBLE_SIZE, COARSE), jnp.float32, 0.6, 1.4)
    weights = scatter_part + jnp.eye(ENSEMBLE_SIZE, dtype=jnp.float32)[:, :, None] * diagonal_part[:, None, :]
    return weights.reshape(ENSEMBLE_SIZE * ENSEMBLE_SIZE, COARSE).astype(jnp.float32)


def place_ends(drawn, stream_key, smallest, high):
    spot = [jax.random.randint(jax.random.fold_in(stream_key, axis), (), 0, length) for axis, length in enumerate(drawn.shape)]
    widest = drawn.shape.index(max(drawn.shape))
    next_to = spot[:widest] + [(spot[widest] + 1) % drawn.shape[widest]] + spot[widest + 1:]
    return drawn.at[tuple(spot)].set(smallest).at[tuple(next_to)].set(high)


def shard_levels(rng, dims, cuts, low, top_value):
    factor_of = 1.0
    for dim, parts in cuts:
        steps = jax.random.uniform(jax.random.fold_in(jax.random.fold_in(rng, 6), dim), (parts,), jnp.float32, low / len(cuts), top_value / len(cuts))
        factor_of = factor_of * jnp.repeat(jnp.exp(steps), dims[dim] // parts).reshape((-1,) + (1,) * (len(dims) - 1 - dim))
    return factor_of


def scatter_about(stream_key, shape, scale, limit, pieces=(), kind=jnp.bfloat16):
    gain = shard_levels(stream_key, shape, pieces, -0.22, 0.18) if pieces else 1.0
    entries = jax.random.normal(stream_key, shape, jnp.float32) * scale * gain
    return jnp.minimum(jnp.maximum(entries, -limit), limit).astype(kind)


def setup_inputs(seed: int = 0) -> dict:
    seeds = jax.random.split(jax.random.key(seed), 6)
    return {
        "prior_ensemble": scatter_about(seeds[0], (ENSEMBLE_SIZE, STATE_QUANTITIES, MESH_SITES), 1.0, 6.0, ((0, 4), (2, 8))),
        "domain_site_mapping": draw_domain_site_mapping(jax.random.fold_in(seeds[5], 71), 0),
        "neighbour_triples": place_ends(jax.random.randint(seeds[2], (PATCHES, 3, CELLS_DEV), 0, COARSE_DEV + 2 * RIM), jax.random.fold_in(seeds[2], 1), 0, (COARSE_DEV + 2 * RIM) - 1).astype(jnp.int32),
        "stencil_factors": jnp.clip(jnp.exp(math.log(1.0) - 2.3025851 * jax.random.uniform(seeds[3], (PATCHES, 3, CELLS_DEV), jnp.float32) ** shard_levels(seeds[3], (PATCHES, 3, CELLS_DEV), ((0, 8), (2, 4)), -0.2, 0.2)), 0.1, 1.0),
        "sparse_node_transforms": draw_sparse_node_transforms(jax.random.fold_in(seeds[5], 71), 0),
    }


def reference(prior_ensemble, domain_site_mapping, neighbour_triples, stencil_factors, sparse_node_transforms):
    source_base = (jnp.arange(COLUMNS, dtype=jnp.int32) // PER_SOURCE) * CELLS_DEV
    cell_ids = (domain_site_mapping + source_base[None, None, :]).reshape(PATCHES, CELLS_DEV).astype(jnp.int32)

    def one_patch(inputs):
        sites_within_tile, points, raw_share, patch_id = inputs
        arriving_analysis_slots = jnp.take(prior_ensemble, sites_within_tile, axis=2)
        member_mean = jnp.sum(arriving_analysis_slots, axis=0, dtype=jnp.float32) / ENSEMBLE_SIZE
        deviation = (arriving_analysis_slots.astype(jnp.float32) - member_mean[None]).astype(jnp.bfloat16)
        coarse_ids = ((patch_id * COARSE_DEV - RIM + points) % COARSE).astype(jnp.int32)
        shares = raw_share / jnp.sum(raw_share, axis=0, keepdims=True)
        blended = jnp.zeros((ENSEMBLE_SIZE * ENSEMBLE_SIZE, CELLS_DEV), jnp.float32)
        for which in range(3):
            blended = blended + jnp.take(sparse_node_transforms, coarse_ids[which], axis=1) * shares[which][None, :]
        blended = blended.reshape(ENSEMBLE_SIZE, ENSEMBLE_SIZE, CELLS_DEV).astype(jnp.bfloat16)
        result = jnp.einsum('kfc,kjc->jfc', deviation.astype(jnp.float32), blended.astype(jnp.float32)) + member_mean[None]
        return result.astype(jnp.bfloat16)

    patch_list = jnp.arange(PATCHES, dtype=jnp.int32)
    results = lax.map(one_patch, (cell_ids, neighbour_triples, stencil_factors, patch_list))
    ordered = jnp.moveaxis(results, 0, 2).reshape(ENSEMBLE_SIZE, STATE_QUANTITIES, MESH_SITES)
    analysis = jnp.zeros((ENSEMBLE_SIZE, STATE_QUANTITIES, MESH_SITES), jnp.bfloat16)
    analysis = analysis.at[:, :, cell_ids.reshape(-1)].set(ordered)
    return analysis
```

```python
import functools

import jax
import jax.numpy as jnp
from jax import lax
from jax.experimental import pallas as pl
from jax.experimental.pallas import tpu as pltpu
from jax.sharding import PartitionSpec as P

RIM = 16
LANES = 128
MESH = pl.DeviceIdType.MESH


def member_peer(me, r, n):
    if n & (n - 1):
        return lax.rem(me + r, n)
    peer = me
    bit = 1
    while bit < n:
        if r & bit:
            peer = peer + bit * (1 - 2 * lax.rem(me // bit, 2))
        bit *= 2
    return peer


def exchange_kernel(
    groups,
    patches,
    mapping_hbm,
    triples_hbm,
    factors_hbm,
    transforms_hbm,
    prior_hbm,
    out_hbm,
    mapping_ref,
    triples_ref,
    factors_ref,
    t32_ref,
    tall_ref,
    meta_out_ref,
    meta_in_ref,
    meta_ref,
    ids_ref,
    share_ref,
    x_ref,
    dev_ref,
    mean_ref,
    spread_ref,
    w_ref,
    result_ref,
    local_sem,
    own_sem,
    xs_sem,
    xr_sem,
    ts_sem,
    tr_sem,
    fs_sem,
    fr_sem,
    ms_sem,
    mr_sem,
    ns_sem,
    nr_sem,
    os_sem,
    or_sem,
    keep_sem,
):
    me = lax.axis_index("member")
    region = lax.axis_index("grid")
    chunks, _, mine, fields, width = x_ref.shape
    members = mine * groups
    columns = chunks * width
    pairs, coarse = tall_ref.shape
    coarse_dev = coarse // patches
    per_source = mapping_ref.shape[2]
    blocks = columns // LANES
    partner = region + 1 - 2 * lax.rem(region, 2)

    barrier = pltpu.get_barrier_semaphore()
    for r in range(1, groups):
        pl.semaphore_signal(
            barrier, inc=1, device_id={"member": member_peer(me, r, groups)}, device_id_type=MESH
        )
    for d in range(1, patches):
        pl.semaphore_signal(
            barrier, inc=1, device_id={"grid": lax.rem(region + d, patches)}, device_id_type=MESH
        )
    pl.semaphore_wait(barrier, groups + patches - 2)

    def forecast(c, r):
        peer = member_peer(me, r, groups)
        at = pl.ds(pl.multiple_of(peer * columns + c * width, width), width)
        return pltpu.make_async_remote_copy(
            src_ref=prior_hbm.at[:, :, at],
            dst_ref=x_ref.at[c, me],
            send_sem=xs_sem.at[c, r],
            recv_sem=xr_sem.at[c, r],
            device_id={"member": peer},
            device_id_type=MESH,
        )

    def own_forecast(c):
        at = pl.ds(pl.multiple_of(me * columns + c * width, width), width)
        return pltpu.make_async_copy(prior_hbm.at[:, :, at], x_ref.at[c, me], own_sem.at[c])

    def send_forecasts(first, last):
        def some(c, carry):
            for r in range(1, groups):
                forecast(c, r).start()
            return carry

        lax.fori_loop(first, last, some, 0)

    early = (chunks + 1) // 2
    send_forecasts(0, early)

    local = [
        pltpu.make_async_copy(triples_hbm.at[0], triples_ref, local_sem.at[0]),
        pltpu.make_async_copy(factors_hbm.at[0], factors_ref, local_sem.at[1]),
        pltpu.make_async_copy(transforms_hbm, t32_ref, local_sem.at[2]),
        pltpu.make_async_copy(mapping_hbm, mapping_ref, local_sem.at[3]),
    ]
    for copy in local:
        copy.start()
    lax.fori_loop(0, chunks, lambda c, z: (own_forecast(c).start(), z)[1], 0)

    local[0].wait()
    local[1].wait()
    raw = factors_ref[...]
    shares = raw / jnp.sum(raw, axis=0, keepdims=True)
    points = triples_ref[...].astype(jnp.float32)
    here = jnp.zeros((1, per_source), jnp.float32) + region.astype(jnp.float32)
    blank = jnp.zeros((1, per_source), jnp.float32)
    if per_source < LANES:
        meta_out_ref[...] = jnp.zeros_like(meta_out_ref)
    for h in range(patches):
        part = slice(h * per_source, (h + 1) * per_source)
        meta_out_ref[h, :, 0:per_source] = jnp.concatenate(
            [points[:, part], shares[:, part], here, blank], axis=0
        )

    def table(d):
        peer = lax.rem(region + d, patches)
        return pltpu.make_async_remote_copy(
            src_ref=meta_out_ref.at[peer],
            dst_ref=meta_in_ref.at[region],
            send_sem=ms_sem.at[d],
            recv_sem=mr_sem.at[d],
            device_id={"grid": peer},
            device_id_type=MESH,
        )

    for d in range(1, patches):
        table(d).start()
    meta_in_ref[region] = meta_out_ref[region]

    local[2].wait()

    def block_of(q):
        return tall_ref.at[:, pl.ds(pl.multiple_of(q * coarse_dev, coarse_dev), coarse_dev)]

    rows = pairs // 10

    def narrow(i, carry):
        at = pl.ds(pl.multiple_of(i * rows, rows), rows)
        lanes = pl.ds(pl.multiple_of(region * coarse_dev, coarse_dev), coarse_dev)
        tall_ref[at, lanes] = t32_ref[at, :].astype(jnp.bfloat16)
        return carry

    lax.fori_loop(0, 10, narrow, 0)
    half = patches // 2

    def transforms_far(d):
        return pltpu.make_async_remote_copy(
            src_ref=block_of(region),
            dst_ref=block_of(region),
            send_sem=ts_sem.at[d],
            recv_sem=tr_sem.at[d],
            device_id={"grid": lax.rem(region + 2 * d, patches)},
            device_id_type=MESH,
        )

    def transforms_near(d):
        source = lax.rem(region - 2 * d + patches, patches)
        return pltpu.make_async_remote_copy(
            src_ref=block_of(source),
            dst_ref=block_of(source),
            send_sem=fs_sem.at[d],
            recv_sem=fr_sem.at[d],
            device_id={"grid": partner},
            device_id_type=MESH,
        )

    for d in range(1, half):
        transforms_far(d).start()
    transforms_near(0).start()

    for d in range(1, patches):
        table(d).wait_recv()
    for gp in range(half):
        meta_ref[me, gp] = meta_in_ref[2 * gp : 2 * gp + 2].reshape(16, LANES).astype(jnp.bfloat16)

    def tables(r):
        return pltpu.make_async_remote_copy(
            src_ref=meta_ref.at[me],
            dst_ref=meta_ref.at[me],
            send_sem=ns_sem.at[r],
            recv_sem=nr_sem.at[r],
            device_id={"member": member_peer(me, r, groups)},
            device_id_type=MESH,
        )

    for r in range(1, groups):
        tables(r).start()
    send_forecasts(early, chunks)

    def arrive(c):
        own_forecast(c).wait()
        for r in range(1, groups):
            forecast(c, r).wait_recv()

    def center(c):
        for lane in range(0, width, LANES):
            lanes = slice(lane, lane + LANES)

            def add(kk, total, lanes=lanes):
                for g in range(groups):
                    total = total + x_ref[c, g, kk, :, lanes].astype(jnp.float32)
                return total

            total = lax.fori_loop(0, mine, add, jnp.zeros((fields, LANES), jnp.float32))
            mean = total / members
            mean_ref[c, :, lanes] = mean

            def less(kk, carry, lanes=lanes, mean=mean):
                for g in range(groups):
                    d = x_ref[c, g, kk, :, lanes].astype(jnp.float32) - mean
                    dev_ref[c, g * mine + kk, :, lanes] = d.astype(jnp.bfloat16).astype(jnp.float32)
                return carry

            lax.fori_loop(0, mine, less, 0)

    def early_center(c, carry):
        arrive(c)
        center(c)
        return carry

    lax.fori_loop(0, early, early_center, 0)

    local[3].wait()
    for r in range(1, groups):
        tables(r).wait_recv()
    cells = lax.broadcasted_iota(jnp.int32, (columns, per_source), 0) + me * columns

    def look(gp, found):
        for m in range(groups):
            both = meta_ref[m, gp]
            if per_source < LANES:
                both = both[:, 0:per_source]
            for side in range(2):
                spots = mapping_ref[2 * gp + side, m : m + 1, :]
                onehot = jnp.where(cells == spots, 1.0, 0.0).astype(jnp.bfloat16)
                hit = lax.dot_general(
                    both, onehot, (((1,), (1,)), ((), ())), preferred_element_type=jnp.float32
                )
                found = found + hit[8 * side : 8 * side + 8]
        return found

    found = lax.fori_loop(0, half, look, jnp.zeros((8, columns), jnp.float32))
    ids = found[0:3] + (found[6:7] * coarse_dev - RIM)
    ids = jnp.where(ids < 0.0, ids + coarse, ids)
    ids = jnp.where(ids >= coarse, ids - coarse, ids)
    for c in range(chunks):
        ids_ref[c, 0:3] = ids[:, c * width : (c + 1) * width]
        share_ref[c, 0:3] = found[3:6, c * width : (c + 1) * width]

    lax.fori_loop(early, chunks - 1, early_center, 0)

    for d in range(1, half):
        transforms_far(d).wait_recv()
        transforms_near(d).start()
    for d in range(half):
        transforms_near(d).wait_recv()

    def result(b, r):
        peer = member_peer(me, r, groups)
        at = pl.ds(pl.multiple_of(me * columns + b * LANES, LANES), LANES)
        return pltpu.make_async_remote_copy(
            src_ref=result_ref.at[b, pl.ds(peer * mine, mine)],
            dst_ref=out_hbm.at[:, :, at],
            send_sem=os_sem.at[b, r],
            recv_sem=or_sem.at[b, r],
            device_id={"member": peer},
            device_id_type=MESH,
        )

    def own_result(b):
        at = pl.ds(pl.multiple_of(me * columns + b * LANES, LANES), LANES)
        return pltpu.make_async_copy(
            result_ref.at[b, pl.ds(me * mine, mine)], out_hbm.at[:, :, at], keep_sem.at[b]
        )

    step = pairs // 4
    unroll = 8

    def update(c, carry):
        @pl.when(c == chunks - 1)
        def _():
            arrive(c)
            center(c)

        def place(q, z):
            at = pl.multiple_of(q * coarse_dev, coarse_dev)
            slots = lax.broadcasted_iota(jnp.int32, (coarse_dev, width), 0) + at
            slots = slots.astype(jnp.float32)
            spread = jnp.zeros((coarse_dev, width), jnp.float32)
            for s in range(3):
                hit = ids_ref[c, s : s + 1, :] == slots
                spread = spread + jnp.where(hit, share_ref[c, s : s + 1, :], 0.0)
            spread_ref[pl.ds(at, coarse_dev), :] = spread.astype(jnp.bfloat16)
            return z

        lax.fori_loop(0, patches, place, 0)

        def blend(i, z):
            at = pl.ds(pl.multiple_of(i * step, step), step)
            part = jnp.dot(tall_ref[at, :], spread_ref[...], preferred_element_type=jnp.float32)
            w_ref[pl.ds(i * (step // 8), step // 8)] = part.reshape(step // 8, 8, width)
            return z

        lax.fori_loop(0, 4, blend, 0)

        for lane in range(0, width, LANES):
            lanes = slice(lane, lane + LANES)
            b = c * (width // LANES) + lane // LANES

            def contract(jg, z, lanes=lanes, b=b):
                for first in (0, 4):

                    def some(kk, accs, first=first):
                        accs = list(accs)
                        for u in range(unroll):
                            k = kk * unroll + u
                            d = dev_ref[c, k, :, lanes]
                            for jj in range(4):
                                row = first + jj
                                w = w_ref[k * (members // 8) + jg, row : row + 1, lanes]
                                accs[jj] = accs[jj] + d * w
                        return tuple(accs)

                    start = tuple(mean_ref[c, :, lanes] for _ in range(4))
                    accs = lax.fori_loop(0, members // unroll, some, start)
                    for jj in range(4):
                        result_ref[b, jg * 8 + first + jj] = accs[jj].astype(jnp.bfloat16)
                return z

            lax.fori_loop(0, members // 8, contract, 0)
            for r in range(1, groups):
                result(b, r).start()
            own_result(b).start()
        return carry

    lax.fori_loop(0, chunks, update, 0)

    for d in range(1, patches):
        table(d).wait_send()
    for r in range(1, groups):
        tables(r).wait_send()
    for d in range(1, half):
        transforms_far(d).wait_send()
    for d in range(half):
        transforms_near(d).wait_send()

    def sent(c, carry):
        for r in range(1, groups):
            forecast(c, r).wait_send()
        return carry

    lax.fori_loop(0, chunks, sent, 0)

    def finish(b, carry):
        own_result(b).wait()
        for r in range(1, groups):
            result(b, r).wait()
        return carry

    lax.fori_loop(0, blocks, finish, 0)


def on_device(prior, mapping, triples, factors, transforms):
    groups = lax.axis_size("member")
    patches = lax.axis_size("grid")
    mine, fields, cells = prior.shape
    members = mine * groups
    columns = cells // groups
    per_source = mapping.shape[2]
    pairs, coarse_dev = transforms.shape
    coarse = coarse_dev * patches
    width = min(256, columns)
    chunks = columns // width
    blocks = columns // LANES
    anywhere = pl.BlockSpec(memory_space=pl.ANY)
    dma = pltpu.SemaphoreType.DMA
    return pl.pallas_call(
        functools.partial(exchange_kernel, groups, patches),
        out_shape=jax.ShapeDtypeStruct(prior.shape, jnp.bfloat16),
        in_specs=[anywhere] * 5,
        out_specs=anywhere,
        scratch_shapes=[
            pltpu.VMEM((patches, groups, per_source), jnp.int32),
            pltpu.VMEM((3, columns), jnp.int32),
            pltpu.VMEM((3, columns), jnp.float32),
            pltpu.VMEM((pairs, coarse_dev), jnp.float32),
            pltpu.VMEM((pairs, coarse), jnp.bfloat16),
            pltpu.VMEM((patches, 8, LANES), jnp.float32),
            pltpu.VMEM((patches, 8, LANES), jnp.float32),
            pltpu.VMEM((groups, patches // 2, 16, LANES), jnp.bfloat16),
            pltpu.VMEM((chunks, 8, width), jnp.float32),
            pltpu.VMEM((chunks, 8, width), jnp.float32),
            pltpu.VMEM((chunks, groups, mine, fields, width), jnp.bfloat16),
            pltpu.VMEM((chunks, members, fields, width), jnp.float32),
            pltpu.VMEM((chunks, fields, width), jnp.float32),
            pltpu.VMEM((coarse, width), jnp.bfloat16),
            pltpu.VMEM((pairs // 8, 8, width), jnp.float32),
            pltpu.VMEM((blocks, members, fields, LANES), jnp.bfloat16),
            dma((4,)),
            dma((chunks,)),
            dma((chunks, groups)),
            dma((chunks, groups)),
            dma((patches // 2,)),
            dma((patches // 2,)),
            dma((patches // 2,)),
            dma((patches // 2,)),
            dma((patches,)),
            dma((patches,)),
            dma((groups,)),
            dma((groups,)),
            dma((blocks, groups)),
            dma((blocks, groups)),
            dma((blocks,)),
        ],
        compiler_params=pltpu.CompilerParams(
            collective_id=0, has_side_effects=True, vmem_limit_bytes=60 * 1024 * 1024
        ),
        name="exchange",
    )(mapping, triples, factors, transforms, prior)


def solution(mesh):
    return jax.shard_map(
        on_device,
        mesh=mesh,
        in_specs=(
            P("member", None, "grid"),
            P(None, None, "grid"),
            P("grid", None, "member"),
            P("grid", None, "member"),
            P(None, "grid"),
        ),
        out_specs=P("member", None, "grid"),
        check_vma=False,
    )
```

```python
import functools

import jax
import jax.numpy as jnp
from jax import lax
from jax.experimental import pallas as pl
from jax.experimental.pallas import tpu as pltpu
from jax.sharding import PartitionSpec as P

RIM = 16
LANES = 128
MESH = pl.DeviceIdType.MESH


def member_peer(me, r, n):
    if n & (n - 1):
        return lax.rem(me + r, n)
    peer = me
    bit = 1
    while bit < n:
        if r & bit:
            peer = peer + bit * (1 - 2 * lax.rem(me // bit, 2))
        bit *= 2
    return peer


def exchange_kernel(
    groups,
    patches,
    mapping_hbm,
    triples_hbm,
    factors_hbm,
    transforms_hbm,
    prior_hbm,
    out_hbm,
    mapping_ref,
    triples_ref,
    factors_ref,
    t32_ref,
    tall_ref,
    meta_out_ref,
    meta_in_ref,
    meta_ref,
    ids_ref,
    share_ref,
    x_ref,
    dev_ref,
    mean_ref,
    spread_ref,
    w_ref,
    result_ref,
    local_sem,
    own_sem,
    xs_sem,
    xr_sem,
    ts_sem,
    tr_sem,
    fs_sem,
    fr_sem,
    ms_sem,
    mr_sem,
    ns_sem,
    nr_sem,
    os_sem,
    or_sem,
):
    me = lax.axis_index("member")
    region = lax.axis_index("grid")
    chunks, _, mine, fields, width = x_ref.shape
    members = mine * groups
    columns = chunks * width
    pairs, coarse = tall_ref.shape
    coarse_dev = coarse // patches
    per_source = mapping_ref.shape[2]
    blocks = columns // LANES
    partner = region + 1 - 2 * lax.rem(region, 2)

    barrier = pltpu.get_barrier_semaphore()
    for r in range(1, groups):
        pl.semaphore_signal(
            barrier, inc=1, device_id={"member": member_peer(me, r, groups)}, device_id_type=MESH
        )
    for d in range(1, patches):
        pl.semaphore_signal(
            barrier, inc=1, device_id={"grid": lax.rem(region + d, patches)}, device_id_type=MESH
        )
    pl.semaphore_wait(barrier, groups + patches - 2)

    def forecast(c, r):
        peer = member_peer(me, r, groups)
        at = pl.ds(pl.multiple_of(peer * columns + c * width, width), width)
        return pltpu.make_async_remote_copy(
            src_ref=prior_hbm.at[:, :, at],
            dst_ref=x_ref.at[c, me],
            send_sem=xs_sem.at[c, r],
            recv_sem=xr_sem.at[c, r],
            device_id={"member": peer},
            device_id_type=MESH,
        )

    def own_forecast(c):
        at = pl.ds(pl.multiple_of(me * columns + c * width, width), width)
        return pltpu.make_async_copy(prior_hbm.at[:, :, at], x_ref.at[c, me], own_sem.at[c])

    def send_forecasts(first, last):
        def some(c, carry):
            for r in range(1, groups):
                forecast(c, r).start()
            return carry

        lax.fori_loop(first, last, some, 0)

    early = (chunks + 1) // 2
    send_forecasts(0, early)

    local = [
        pltpu.make_async_copy(triples_hbm.at[:, 0], triples_ref, local_sem.at[0]),
        pltpu.make_async_copy(factors_hbm.at[:, 0], factors_ref, local_sem.at[1]),
        pltpu.make_async_copy(transforms_hbm, t32_ref, local_sem.at[2]),
        pltpu.make_async_copy(mapping_hbm, mapping_ref, local_sem.at[3]),
    ]
    for copy in local:
        copy.start()
    lax.fori_loop(0, chunks, lambda c, z: (own_forecast(c).start(), z)[1], 0)

    local[0].wait()
    local[1].wait()
    raw = factors_ref[...]
    shares = raw / jnp.sum(raw, axis=0, keepdims=True)
    points = triples_ref[...].astype(jnp.float32)
    here = jnp.zeros((1, per_source), jnp.float32) + region.astype(jnp.float32)
    blank = jnp.zeros((1, per_source), jnp.float32)
    if per_source < LANES:
        meta_out_ref[...] = jnp.zeros_like(meta_out_ref)
    for h in range(patches):
        part = slice(h * per_source, (h + 1) * per_source)
        meta_out_ref[h, :, 0:per_source] = jnp.concatenate(
            [points[:, part], shares[:, part], here, blank], axis=0
        )

    def table(d):
        peer = lax.rem(region + d, patches)
        return pltpu.make_async_remote_copy(
            src_ref=meta_out_ref.at[peer],
            dst_ref=meta_in_ref.at[region],
            send_sem=ms_sem.at[d],
            recv_sem=mr_sem.at[d],
            device_id={"grid": peer},
            device_id_type=MESH,
        )

    for d in range(1, patches):
        table(d).start()
    meta_in_ref[region] = meta_out_ref[region]

    local[2].wait()

    def block_of(q):
        return tall_ref.at[:, pl.ds(pl.multiple_of(q * coarse_dev, coarse_dev), coarse_dev)]

    rows = pairs // 10

    def narrow(i, carry):
        at = pl.ds(pl.multiple_of(i * rows, rows), rows)
        lanes = pl.ds(pl.multiple_of(region * coarse_dev, coarse_dev), coarse_dev)
        tall_ref[at, lanes] = t32_ref[at, :].astype(jnp.bfloat16)
        return carry

    lax.fori_loop(0, 10, narrow, 0)
    half = patches // 2

    def transforms_far(d):
        return pltpu.make_async_remote_copy(
            src_ref=block_of(region),
            dst_ref=block_of(region),
            send_sem=ts_sem.at[d],
            recv_sem=tr_sem.at[d],
            device_id={"grid": lax.rem(region + 2 * d, patches)},
            device_id_type=MESH,
        )

    def transforms_near(d):
        source = lax.rem(region - 2 * d + patches, patches)
        return pltpu.make_async_remote_copy(
            src_ref=block_of(source),
            dst_ref=block_of(source),
            send_sem=fs_sem.at[d],
            recv_sem=fr_sem.at[d],
            device_id={"grid": partner},
            device_id_type=MESH,
        )

    for d in range(1, half):
        transforms_far(d).start()
    transforms_near(0).start()

    for d in range(1, patches):
        table(d).wait_recv()
    for gp in range(half):
        meta_ref[me, gp] = meta_in_ref[2 * gp : 2 * gp + 2].reshape(16, LANES).astype(jnp.bfloat16)

    def tables(r):
        return pltpu.make_async_remote_copy(
            src_ref=meta_ref.at[me],
            dst_ref=meta_ref.at[me],
            send_sem=ns_sem.at[r],
            recv_sem=nr_sem.at[r],
            device_id={"member": member_peer(me, r, groups)},
            device_id_type=MESH,
        )

    for r in range(1, groups):
        tables(r).start()
    send_forecasts(early, chunks)

    def arrive(c):
        own_forecast(c).wait()
        for r in range(1, groups):
            forecast(c, r).wait_recv()

    def center(c):
        for lane in range(0, width, LANES):
            lanes = slice(lane, lane + LANES)

            def add(kk, total, lanes=lanes):
                for g in range(groups):
                    total = total + x_ref[c, g, kk, :, lanes].astype(jnp.float32)
                return total

            total = lax.fori_loop(0, mine, add, jnp.zeros((fields, LANES), jnp.float32))
            mean = total / members
            mean_ref[c, :, lanes] = mean

            def less(kk, carry, lanes=lanes, mean=mean):
                for g in range(groups):
                    d = x_ref[c, g, kk, :, lanes].astype(jnp.float32) - mean
                    dev_ref[c, g * mine + kk, :, lanes] = d.astype(jnp.bfloat16).astype(jnp.float32)
                return carry

            lax.fori_loop(0, mine, less, 0)

    def early_center(c, carry):
        arrive(c)
        center(c)
        return carry

    lax.fori_loop(0, early, early_center, 0)

    local[3].wait()
    for r in range(1, groups):
        tables(r).wait_recv()
    cells = lax.broadcasted_iota(jnp.int32, (columns, per_source), 0) + me * columns

    def look(gp, found):
        for m in range(groups):
            both = meta_ref[m, gp]
            if per_source < LANES:
                both = both[:, 0:per_source]
            for side in range(2):
                spots = mapping_ref[2 * gp + side, m : m + 1, :]
                onehot = jnp.where(cells == spots, 1.0, 0.0).astype(jnp.bfloat16)
                hit = lax.dot_general(
                    both, onehot, (((1,), (1,)), ((), ())), preferred_element_type=jnp.float32
                )
                found = found + hit[8 * side : 8 * side + 8]
        return found

    found = lax.fori_loop(0, half, look, jnp.zeros((8, columns), jnp.float32))
    ids = found[0:3] + (found[6:7] * coarse_dev - RIM)
    ids = jnp.where(ids < 0.0, ids + coarse, ids)
    ids = jnp.where(ids >= coarse, ids - coarse, ids)
    for c in range(chunks):
        ids_ref[c, 0:3] = ids[:, c * width : (c + 1) * width]
        share_ref[c, 0:3] = found[3:6, c * width : (c + 1) * width]

    lax.fori_loop(early, chunks - 1, early_center, 0)

    for d in range(1, half):
        transforms_far(d).wait_recv()
        transforms_near(d).start()
    for d in range(half):
        transforms_near(d).wait_recv()

    def result(b, r):
        peer = member_peer(me, r, groups)
        at = pl.ds(pl.multiple_of(me * columns + b * LANES, LANES), LANES)
        return pltpu.make_async_remote_copy(
            src_ref=result_ref.at[b, pl.ds(peer * mine, mine)],
            dst_ref=out_hbm.at[:, :, at],
            send_sem=os_sem.at[b, r],
            recv_sem=or_sem.at[b, r],
            device_id={"member": peer},
            device_id_type=MESH,
        )

    def own_result(b):
        at = pl.ds(pl.multiple_of(me * columns + b * LANES, LANES), LANES)

        def put(kk, carry):
            out_hbm[kk, :, at] = result_ref[b, me * mine + kk]
            return carry

        lax.fori_loop(0, mine, put, 0)

    step = pairs // 4
    unroll = 8

    def update(c, carry):
        @pl.when(c == chunks - 1)
        def _():
            arrive(c)
            center(c)

        def place(q, z):
            at = pl.multiple_of(q * coarse_dev, coarse_dev)
            slots = lax.broadcasted_iota(jnp.int32, (coarse_dev, width), 0) + at
            slots = slots.astype(jnp.float32)
            spread = jnp.zeros((coarse_dev, width), jnp.float32)
            for s in range(3):
                hit = ids_ref[c, s : s + 1, :] == slots
                spread = spread + jnp.where(hit, share_ref[c, s : s + 1, :], 0.0)
            spread_ref[pl.ds(at, coarse_dev), :] = spread.astype(jnp.bfloat16)
            return z

        lax.fori_loop(0, patches, place, 0)

        def blend(i, z):
            at = pl.ds(pl.multiple_of(i * step, step), step)
            part = jnp.dot(tall_ref[at, :], spread_ref[...], preferred_element_type=jnp.float32)
            w_ref[pl.ds(i * (step // 8), step // 8)] = part.reshape(step // 8, 8, width)
            return z

        lax.fori_loop(0, 4, blend, 0)

        for lane in range(0, width, LANES):
            lanes = slice(lane, lane + LANES)
            b = c * (width // LANES) + lane // LANES

            def contract(jg, z, lanes=lanes, b=b):
                for first in (0, 4):

                    def some(kk, accs, first=first):
                        accs = list(accs)
                        for u in range(unroll):
                            k = kk * unroll + u
                            d = dev_ref[c, k, :, lanes]
                            for jj in range(4):
                                row = first + jj
                                w = w_ref[k * (members // 8) + jg, row : row + 1, lanes]
                                accs[jj] = accs[jj] + d * w
                        return tuple(accs)

                    start = tuple(mean_ref[c, :, lanes] for _ in range(4))
                    accs = lax.fori_loop(0, members // unroll, some, start)
                    for jj in range(4):
                        result_ref[b, jg * 8 + first + jj] = accs[jj].astype(jnp.bfloat16)
                return z

            lax.fori_loop(0, members // 8, contract, 0)
            for r in range(1, groups):
                result(b, r).start()
            own_result(b)
        return carry

    lax.fori_loop(0, chunks, update, 0)

    for d in range(1, patches):
        table(d).wait_send()
    for r in range(1, groups):
        tables(r).wait_send()
    for d in range(1, half):
        transforms_far(d).wait_send()
    for d in range(half):
        transforms_near(d).wait_send()

    def sent(c, carry):
        for r in range(1, groups):
            forecast(c, r).wait_send()
        return carry

    lax.fori_loop(0, chunks, sent, 0)

    def finish(b, carry):
        for r in range(1, groups):
            result(b, r).wait()
        return carry

    lax.fori_loop(0, blocks, finish, 0)


def on_device(prior, mapping, triples, factors, transforms):
    groups = lax.axis_size("member")
    patches = lax.axis_size("grid")
    mine, fields, cells = prior.shape
    members = mine * groups
    columns = cells // groups
    per_source = mapping.shape[2]
    pairs, coarse_dev = transforms.shape
    coarse = coarse_dev * patches
    width = min(256, columns)
    chunks = columns // width
    blocks = columns // LANES
    anywhere = pl.BlockSpec(memory_space=pl.ANY)
    dma = pltpu.SemaphoreType.DMA
    return pl.pallas_call(
        functools.partial(exchange_kernel, groups, patches),
        out_shape=pltpu.VMEM(prior.shape, jnp.bfloat16),
        in_specs=[anywhere] * 5,
        out_specs=pl.BlockSpec(memory_space=pltpu.VMEM),
        scratch_shapes=[
            pltpu.VMEM((patches, groups, per_source), jnp.int32),
            pltpu.VMEM((3, columns), jnp.int32),
            pltpu.VMEM((3, columns), jnp.float32),
            pltpu.VMEM((pairs, coarse_dev), jnp.float32),
            pltpu.VMEM((pairs, coarse), jnp.bfloat16),
            pltpu.VMEM((patches, 8, LANES), jnp.float32),
            pltpu.VMEM((patches, 8, LANES), jnp.float32),
            pltpu.VMEM((groups, patches // 2, 16, LANES), jnp.bfloat16),
            pltpu.VMEM((chunks, 8, width), jnp.float32),
            pltpu.VMEM((chunks, 8, width), jnp.float32),
            pltpu.VMEM((chunks, groups, mine, fields, width), jnp.bfloat16),
            pltpu.VMEM((chunks, members, fields, width), jnp.float32),
            pltpu.VMEM((chunks, fields, width), jnp.float32),
            pltpu.VMEM((coarse, width), jnp.bfloat16),
            pltpu.VMEM((pairs // 8, 8, width), jnp.float32),
            pltpu.VMEM((blocks, members, fields, LANES), jnp.bfloat16),
            dma((4,)),
            dma((chunks,)),
            dma((chunks, groups)),
            dma((chunks, groups)),
            dma((patches // 2,)),
            dma((patches // 2,)),
            dma((patches // 2,)),
            dma((patches // 2,)),
            dma((patches,)),
            dma((patches,)),
            dma((groups,)),
            dma((groups,)),
            dma((blocks, groups)),
            dma((blocks, groups)),
        ],
        compiler_params=pltpu.CompilerParams(
            collective_id=0, has_side_effects=True, vmem_limit_bytes=44 * 1024 * 1024
        ),
        name="exchange",
    )(*[
        pltpu.with_memory_space_constraint(a, pltpu.HBM)
        for a in (
            mapping,
            jnp.transpose(triples, (1, 0, 2)),
            jnp.transpose(factors, (1, 0, 2)),
            transforms,
            prior,
        )
    ])


def solution(mesh):
    return jax.shard_map(
        on_device,
        mesh=mesh,
        in_specs=(
            P("member", None, "grid"),
            P(None, None, "grid"),
            P("grid", None, "member"),
            P("grid", None, "member"),
            P(None, "grid"),
        ),
        out_specs=P("member", None, "grid"),
        check_vma=False,
    )
```

```python
import functools

import jax
import jax.numpy as jnp
from jax import lax
from jax.experimental import pallas as pl
from jax.experimental.pallas import tpu as pltpu
from jax.sharding import PartitionSpec as P

RIM = 16
LANES = 128
MESH = pl.DeviceIdType.MESH


def member_peer(me, r, n):
    if n & (n - 1):
        return lax.rem(me + r, n)
    peer = me
    bit = 1
    while bit < n:
        if r & bit:
            peer = peer + bit * (1 - 2 * lax.rem(me // bit, 2))
        bit *= 2
    return peer


def exchange_kernel(
    groups,
    patches,
    mapping_hbm,
    triples_hbm,
    factors_hbm,
    transforms_hbm,
    prior_hbm,
    out_hbm,
    mapping_ref,
    triples_ref,
    factors_ref,
    t32_ref,
    tall_ref,
    meta_out_ref,
    meta_in_ref,
    meta_ref,
    ids_ref,
    share_ref,
    x_ref,
    dev_ref,
    mean_ref,
    spread_ref,
    w_ref,
    result_ref,
    local_sem,
    own_sem,
    xs_sem,
    xr_sem,
    near_sem,
    far_sem,
    ts_sem,
    tr_sem,
    fs_sem,
    fr_sem,
    ms_sem,
    mr_sem,
    ns_sem,
    nr_sem,
    os_sem,
    or_sem,
):
    me = lax.axis_index("member")
    region = lax.axis_index("grid")
    chunks, _, mine, fields, width = x_ref.shape
    members = mine * groups
    columns = chunks * width
    pairs, coarse = tall_ref.shape
    coarse_dev = coarse // patches
    per_source = mapping_ref.shape[2]
    blocks = columns // LANES
    partner = region + 1 - 2 * lax.rem(region, 2)

    core = lax.rem(region, 2)
    spot = region // 2
    spots = patches // 2
    barrier = pltpu.get_barrier_semaphore()
    for r in range(groups):
        hub = {"member": member_peer(me, r, groups), "grid": 2 * spot + 1}
        if r:
            pl.semaphore_signal(barrier, inc=1, device_id=hub, device_id_type=MESH)
        else:

            @pl.when(core == 0)
            def _(hub=hub):
                pl.semaphore_signal(barrier, inc=1, device_id=hub, device_id_type=MESH)

    @pl.when(core == 1)
    def _():
        pl.semaphore_wait(barrier, 2 * groups - 1)
        pl.semaphore_signal(near_sem, inc=1, device_id={"grid": partner}, device_id_type=MESH)

    @pl.when(core == 0)
    def _():
        pl.semaphore_wait(near_sem, 1)
        for d in range(1, spots):
            other = 2 * lax.rem(spot + d, spots)
            pl.semaphore_signal(barrier, inc=1, device_id={"grid": other}, device_id_type=MESH)

    def meet_grid():
        @pl.when(core == 0)
        def _():
            pl.semaphore_wait(barrier, spots - 1)
            pl.semaphore_signal(far_sem, inc=1, device_id={"grid": partner}, device_id_type=MESH)

        @pl.when(core == 1)
        def _():
            pl.semaphore_wait(far_sem, 1)

    def forecast(c, r):
        peer = member_peer(me, r, groups)
        at = pl.ds(pl.multiple_of(peer * columns + c * width, width), width)
        return pltpu.make_async_remote_copy(
            src_ref=prior_hbm.at[:, :, at],
            dst_ref=x_ref.at[c, me],
            send_sem=xs_sem.at[c, r],
            recv_sem=xr_sem.at[c, r],
            device_id={"member": peer},
            device_id_type=MESH,
        )

    def own_forecast(c):
        at = pl.ds(pl.multiple_of(me * columns + c * width, width), width)
        return pltpu.make_async_copy(prior_hbm.at[:, :, at], x_ref.at[c, me], own_sem.at[c])

    def send_forecasts(first, last):
        def some(c, carry):
            for r in range(1, groups):
                forecast(c, r).start()
            return carry

        lax.fori_loop(first, last, some, 0)

    early = (chunks + 1) // 2
    send_forecasts(0, early)

    local = [
        pltpu.make_async_copy(triples_hbm.at[:, 0], triples_ref, local_sem.at[0]),
        pltpu.make_async_copy(factors_hbm.at[:, 0], factors_ref, local_sem.at[1]),
        pltpu.make_async_copy(transforms_hbm, t32_ref, local_sem.at[2]),
        pltpu.make_async_copy(mapping_hbm, mapping_ref, local_sem.at[3]),
    ]
    for copy in local:
        copy.start()
    lax.fori_loop(0, chunks, lambda c, z: (own_forecast(c).start(), z)[1], 0)

    local[0].wait()
    local[1].wait()
    raw = factors_ref[...]
    shares = raw / jnp.sum(raw, axis=0, keepdims=True)
    points = triples_ref[...].astype(jnp.float32)
    here = jnp.zeros((1, per_source), jnp.float32) + region.astype(jnp.float32)
    blank = jnp.zeros((1, per_source), jnp.float32)
    if per_source < LANES:
        meta_out_ref[...] = jnp.zeros_like(meta_out_ref)
    for h in range(patches):
        part = slice(h * per_source, (h + 1) * per_source)
        meta_out_ref[h, :, 0:per_source] = jnp.concatenate(
            [points[:, part], shares[:, part], here, blank], axis=0
        )

    def table(d):
        peer = lax.rem(region + d, patches)
        return pltpu.make_async_remote_copy(
            src_ref=meta_out_ref.at[peer],
            dst_ref=meta_in_ref.at[region],
            send_sem=ms_sem.at[d],
            recv_sem=mr_sem.at[d],
            device_id={"grid": peer},
            device_id_type=MESH,
        )

    local[2].wait()

    def block_of(q):
        return tall_ref.at[:, pl.ds(pl.multiple_of(q * coarse_dev, coarse_dev), coarse_dev)]

    rows = pairs // 10

    def narrow(i, carry):
        at = pl.ds(pl.multiple_of(i * rows, rows), rows)
        lanes = pl.ds(pl.multiple_of(region * coarse_dev, coarse_dev), coarse_dev)
        tall_ref[at, lanes] = t32_ref[at, :].astype(jnp.bfloat16)
        return carry

    lax.fori_loop(0, 10, narrow, 0)
    def along(way, s):
        block = block_of(region - 2 * way * s)
        return pltpu.make_async_remote_copy(
            src_ref=block,
            dst_ref=block,
            send_sem=ts_sem.at[(1 + way) // 2, s],
            recv_sem=tr_sem.at[(1 + way) // 2, s],
            device_id={"grid": region + 2 * way},
            device_id_type=MESH,
        )

    def across(at):
        block = block_of(2 * at + core)
        return pltpu.make_async_remote_copy(
            src_ref=block,
            dst_ref=block,
            send_sem=fs_sem.at[at],
            recv_sem=fr_sem.at[at],
            device_id={"grid": partner},
            device_id_type=MESH,
        )

    def has_next(way):
        return spot + 1 < spots if way == 1 else spot > 0

    def has_source(way, s):
        return spot >= s if way == 1 else spot + s < spots

    def relay(s):
        for way in (1, -1):

            @pl.when(has_source(way, s))
            def _(way=way):
                along(way, s - 1).wait_recv()

                @pl.when(has_next(way))
                def _():
                    along(way, s).start()

                across(spot - way * s).start()

    meet_grid()
    for d in range(1, patches):
        table(d).start()
    meta_in_ref[region] = meta_out_ref[region]

    for way in (1, -1):

        @pl.when(has_next(way))
        def _(way=way):
            along(way, 0).start()

    across(spot).start()

    for d in range(1, patches):
        table(d).wait_recv()
    for gp in range(spots):
        meta_ref[me, gp] = meta_in_ref[2 * gp : 2 * gp + 2].reshape(16, LANES).astype(jnp.bfloat16)

    def tables(r):
        return pltpu.make_async_remote_copy(
            src_ref=meta_ref.at[me],
            dst_ref=meta_ref.at[me],
            send_sem=ns_sem.at[r],
            recv_sem=nr_sem.at[r],
            device_id={"member": member_peer(me, r, groups)},
            device_id_type=MESH,
        )

    for r in range(1, groups):
        tables(r).start()
    send_forecasts(early, chunks)

    def arrive(c):
        own_forecast(c).wait()
        for r in range(1, groups):
            forecast(c, r).wait_recv()

    def center(c):
        for lane in range(0, width, LANES):
            lanes = slice(lane, lane + LANES)

            def add(kk, total, lanes=lanes):
                for g in range(groups):
                    total = total + x_ref[c, g, kk, :, lanes].astype(jnp.float32)
                return total

            total = lax.fori_loop(0, mine, add, jnp.zeros((fields, LANES), jnp.float32))
            mean = total / members
            mean_ref[c, :, lanes] = mean

            def less(kk, carry, lanes=lanes, mean=mean):
                for g in range(groups):
                    d = x_ref[c, g, kk, :, lanes].astype(jnp.float32) - mean
                    dev_ref[c, g * mine + kk, :, lanes] = d.astype(jnp.bfloat16).astype(jnp.float32)
                return carry

            lax.fori_loop(0, mine, less, 0)

    def early_center(c, carry):
        arrive(c)
        center(c)
        return carry

    early_center(0, 0)
    for step_along in range(1, (spots + 1) // 2 + 1):
        relay(step_along)
    lax.fori_loop(1, early, early_center, 0)

    local[3].wait()
    for r in range(1, groups):
        tables(r).wait_recv()
    cells = lax.broadcasted_iota(jnp.int32, (columns, per_source), 0) + me * columns

    def look(gp, found):
        for m in range(groups):
            both = meta_ref[m, gp]
            if per_source < LANES:
                both = both[:, 0:per_source]
            for side in range(2):
                spots = mapping_ref[2 * gp + side, m : m + 1, :]
                onehot = jnp.where(cells == spots, 1.0, 0.0).astype(jnp.bfloat16)
                hit = lax.dot_general(
                    both, onehot, (((1,), (1,)), ((), ())), preferred_element_type=jnp.float32
                )
                found = found + hit[8 * side : 8 * side + 8]
        return found

    found = lax.fori_loop(0, spots, look, jnp.zeros((8, columns), jnp.float32))
    ids = found[0:3] + (found[6:7] * coarse_dev - RIM)
    ids = jnp.where(ids < 0.0, ids + coarse, ids)
    ids = jnp.where(ids >= coarse, ids - coarse, ids)
    for c in range(chunks):
        ids_ref[c, 0:3] = ids[:, c * width : (c + 1) * width]
        share_ref[c, 0:3] = found[3:6, c * width : (c + 1) * width]

    for step_along in range((spots + 1) // 2 + 1, spots):
        relay(step_along)
    for at in range(spots):
        across(at).wait_recv()

    def result(b, r):
        peer = member_peer(me, r, groups)
        at = pl.ds(pl.multiple_of(me * columns + b * LANES, LANES), LANES)
        return pltpu.make_async_remote_copy(
            src_ref=result_ref.at[b, pl.ds(peer * mine, mine)],
            dst_ref=out_hbm.at[:, :, at],
            send_sem=os_sem.at[b, r],
            recv_sem=or_sem.at[b, r],
            device_id={"member": peer},
            device_id_type=MESH,
        )

    def own_result(b):
        at = pl.ds(pl.multiple_of(me * columns + b * LANES, LANES), LANES)

        def put(kk, carry):
            out_hbm[kk, :, at] = result_ref[b, me * mine + kk]
            return carry

        lax.fori_loop(0, mine, put, 0)

    step = pairs // 4
    unroll = 8

    def update(c, carry):
        @pl.when(c >= early)
        def _():
            arrive(c)
            center(c)

        def place(q, z):
            at = pl.multiple_of(q * coarse_dev, coarse_dev)
            slots = lax.broadcasted_iota(jnp.int32, (coarse_dev, width), 0) + at
            slots = slots.astype(jnp.float32)
            spread = jnp.zeros((coarse_dev, width), jnp.float32)
            for s in range(3):
                hit = ids_ref[c, s : s + 1, :] == slots
                spread = spread + jnp.where(hit, share_ref[c, s : s + 1, :], 0.0)
            spread_ref[pl.ds(at, coarse_dev), :] = spread.astype(jnp.bfloat16)
            return z

        lax.fori_loop(0, patches, place, 0)

        def blend(i, z):
            at = pl.ds(pl.multiple_of(i * step, step), step)
            part = jnp.dot(tall_ref[at, :], spread_ref[...], preferred_element_type=jnp.float32)
            w_ref[pl.ds(i * (step // 8), step // 8)] = part.reshape(step // 8, 8, width)
            return z

        lax.fori_loop(0, 4, blend, 0)

        for lane in range(0, width, LANES):
            lanes = slice(lane, lane + LANES)
            b = c * (width // LANES) + lane // LANES

            def contract(jg, z, lanes=lanes, b=b):
                for first in (0, 4):

                    def some(kk, accs, first=first):
                        accs = list(accs)
                        for u in range(unroll):
                            k = kk * unroll + u
                            d = dev_ref[c, k, :, lanes]
                            for jj in range(4):
                                row = first + jj
                                w = w_ref[k * (members // 8) + jg, row : row + 1, lanes]
                                accs[jj] = accs[jj] + d * w
                        return tuple(accs)

                    start = tuple(mean_ref[c, :, lanes] for _ in range(4))
                    accs = lax.fori_loop(0, members // unroll, some, start)
                    for jj in range(4):
                        result_ref[b, jg * 8 + first + jj] = accs[jj].astype(jnp.bfloat16)
                return z

            lax.fori_loop(0, members // 8, contract, 0)
            for r in range(1, groups):
                result(b, r).start()
            own_result(b)
        return carry

    lax.fori_loop(0, chunks, update, 0)

    for d in range(1, patches):
        table(d).wait_send()
    for r in range(1, groups):
        tables(r).wait_send()
    for s in range(spots - 1):
        for way in (1, -1):

            @pl.when(has_next(way) & has_source(way, s))
            def _(way=way, s=s):
                along(way, s).wait_send()

    for at in range(spots):
        across(at).wait_send()

    def sent(c, carry):
        for r in range(1, groups):
            forecast(c, r).wait_send()
        return carry

    lax.fori_loop(0, chunks, sent, 0)

    def finish(b, carry):
        for r in range(1, groups):
            result(b, r).wait()
        return carry

    lax.fori_loop(0, blocks, finish, 0)


def on_device(prior, mapping, triples, factors, transforms):
    groups = lax.axis_size("member")
    patches = lax.axis_size("grid")
    mine, fields, cells = prior.shape
    members = mine * groups
    columns = cells // groups
    per_source = mapping.shape[2]
    pairs, coarse_dev = transforms.shape
    coarse = coarse_dev * patches
    width = min(256, columns)
    chunks = columns // width
    blocks = columns // LANES
    anywhere = pl.BlockSpec(memory_space=pl.ANY)
    dma = pltpu.SemaphoreType.DMA
    return pl.pallas_call(
        functools.partial(exchange_kernel, groups, patches),
        out_shape=pltpu.VMEM(prior.shape, jnp.bfloat16),
        in_specs=[anywhere] * 5,
        out_specs=pl.BlockSpec(memory_space=pltpu.VMEM),
        scratch_shapes=[
            pltpu.VMEM((patches, groups, per_source), jnp.int32),
            pltpu.VMEM((3, columns), jnp.int32),
            pltpu.VMEM((3, columns), jnp.float32),
            pltpu.VMEM((pairs, coarse_dev), jnp.float32),
            pltpu.VMEM((pairs, coarse), jnp.bfloat16),
            pltpu.VMEM((patches, 8, LANES), jnp.float32),
            pltpu.VMEM((patches, 8, LANES), jnp.float32),
            pltpu.VMEM((groups, patches // 2, 16, LANES), jnp.bfloat16),
            pltpu.VMEM((chunks, 8, width), jnp.float32),
            pltpu.VMEM((chunks, 8, width), jnp.float32),
            pltpu.VMEM((chunks, groups, mine, fields, width), jnp.bfloat16),
            pltpu.VMEM((chunks, members, fields, width), jnp.float32),
            pltpu.VMEM((chunks, fields, width), jnp.float32),
            pltpu.VMEM((coarse, width), jnp.bfloat16),
            pltpu.VMEM((pairs // 8, 8, width), jnp.float32),
            pltpu.VMEM((blocks, members, fields, LANES), jnp.bfloat16),
            dma((4,)),
            dma((chunks,)),
            dma((chunks, groups)),
            dma((chunks, groups)),
            pltpu.SemaphoreType.REGULAR,
            pltpu.SemaphoreType.REGULAR,
            dma((2, patches // 2)),
            dma((2, patches // 2)),
            dma((patches // 2,)),
            dma((patches // 2,)),
            dma((patches,)),
            dma((patches,)),
            dma((groups,)),
            dma((groups,)),
            dma((blocks, groups)),
            dma((blocks, groups)),
        ],
        compiler_params=pltpu.CompilerParams(
            collective_id=0, has_side_effects=True, vmem_limit_bytes=44 * 1024 * 1024
        ),
        name="exchange",
    )(*[
        pltpu.with_memory_space_constraint(a, pltpu.HBM)
        for a in (
            mapping,
            jnp.transpose(triples, (1, 0, 2)),
            jnp.transpose(factors, (1, 0, 2)),
            transforms,
            prior,
        )
    ])


def solution(mesh):
    return jax.shard_map(
        on_device,
        mesh=mesh,
        in_specs=(
            P("member", None, "grid"),
            P(None, None, "grid"),
            P("grid", None, "member"),
            P("grid", None, "member"),
            P(None, "grid"),
        ),
        out_specs=P("member", None, "grid"),
        check_vma=False,
    )
```

```python
import functools

import jax
import jax.numpy as jnp
from jax import lax
from jax.experimental import pallas as pl
from jax.experimental.pallas import tpu as pltpu
from jax.sharding import PartitionSpec as P

RIM = 16
LANES = 128
MESH = pl.DeviceIdType.MESH


def member_peer(me, r, n):
    if n & (n - 1):
        return lax.rem(me + r, n)
    peer = me
    bit = 1
    while bit < n:
        if r & bit:
            peer = peer + bit * (1 - 2 * lax.rem(me // bit, 2))
        bit *= 2
    return peer


def exchange_kernel(
    groups,
    patches,
    mapping_hbm,
    triples_hbm,
    factors_hbm,
    transforms_hbm,
    prior_hbm,
    out_hbm,
    mapping_ref,
    triples_ref,
    factors_ref,
    t32_ref,
    tall_ref,
    meta_out_ref,
    meta_in_ref,
    meta_ref,
    ids_ref,
    share_ref,
    x_ref,
    dev_ref,
    mean_ref,
    spread_ref,
    w_ref,
    result_ref,
    stage_ref,
    local_sem,
    stage_sem,
    xs_sem,
    xr_sem,
    near_sem,
    far_sem,
    ts_sem,
    tr_sem,
    fs_sem,
    fr_sem,
    ms_sem,
    mr_sem,
    ns_sem,
    nr_sem,
    os_sem,
    or_sem,
):
    me = lax.axis_index("member")
    region = lax.axis_index("grid")
    chunks, _, mine, fields, width = x_ref.shape
    members = mine * groups
    columns = chunks * width
    pairs, coarse = tall_ref.shape
    coarse_dev = coarse // patches
    per_source = mapping_ref.shape[2]
    partner = region + 1 - 2 * lax.rem(region, 2)

    core = lax.rem(region, 2)
    spot = region // 2
    spots = patches // 2
    barrier = pltpu.get_barrier_semaphore()
    for r in range(groups):
        hub = {"member": member_peer(me, r, groups), "grid": 2 * spot + 1}
        if r:
            pl.semaphore_signal(barrier, inc=1, device_id=hub, device_id_type=MESH)
        else:

            @pl.when(core == 0)
            def _(hub=hub):
                pl.semaphore_signal(barrier, inc=1, device_id=hub, device_id_type=MESH)

    def meet_grid():
        @pl.when(core == 0)
        def _():
            pl.semaphore_wait(barrier, spots - 1)
            pl.semaphore_signal(far_sem, inc=1, device_id={"grid": partner}, device_id_type=MESH)

        @pl.when(core == 1)
        def _():
            pl.semaphore_wait(far_sem, 1)

    def forecast(c, r, staged=False):
        peer = member_peer(me, r, groups)
        at = pl.ds(pl.multiple_of(peer * columns + c * width, width), width)
        return pltpu.make_async_remote_copy(
            src_ref=stage_ref.at[r - 1] if staged else prior_hbm.at[:, :, at],
            dst_ref=x_ref.at[c, me],
            send_sem=xs_sem,
            recv_sem=xr_sem.at[c],
            device_id={"member": peer},
            device_id_type=MESH,
        )

    def send_forecasts(first, last):
        def some(c, carry):
            for r in range(1, groups):
                forecast(c, r).start()
            return carry

        lax.fori_loop(first, last, some, 0)

    def arrived(ref, sem):
        pltpu.make_async_copy(ref, ref, sem).wait()

    early = (chunks + 1) // 2
    for r in range(1, groups):
        at = pl.ds(pl.multiple_of(member_peer(me, r, groups) * columns, width), width)
        pltpu.make_async_copy(prior_hbm.at[:, :, at], stage_ref.at[r - 1], stage_sem).start()
    local = [
        pltpu.make_async_copy(triples_hbm.at[:, 0], triples_ref, local_sem.at[0]),
        pltpu.make_async_copy(factors_hbm.at[:, 0], factors_ref, local_sem.at[1]),
        pltpu.make_async_copy(transforms_hbm, t32_ref, local_sem.at[2]),
        pltpu.make_async_copy(mapping_hbm, mapping_ref, local_sem.at[3]),
    ]
    for copy in local:
        copy.start()
    arrived(stage_ref, stage_sem)

    @pl.when(core == 1)
    def _():
        pl.semaphore_wait(barrier, 2 * groups - 1)
        pl.semaphore_signal(near_sem, inc=1, device_id={"grid": partner}, device_id_type=MESH)

    @pl.when(core == 0)
    def _():
        pl.semaphore_wait(near_sem, 1)
        for d in range(1, spots):
            other = 2 * lax.rem(spot + d, spots)
            pl.semaphore_signal(barrier, inc=1, device_id={"grid": other}, device_id_type=MESH)

    for r in range(1, groups):
        forecast(0, r, True).start()
    send_forecasts(1, early)

    def own_forecast(c, carry):
        at = pl.ds(pl.multiple_of(me * columns + c * width, width), width)
        pltpu.make_async_copy(prior_hbm.at[:, :, at], x_ref.at[c, me], xr_sem.at[c]).start()
        return carry

    lax.fori_loop(0, chunks, own_forecast, 0)

    local[0].wait()
    local[1].wait()
    raw = factors_ref[...]
    shares = raw / jnp.sum(raw, axis=0, keepdims=True)
    points = triples_ref[...].astype(jnp.float32)
    here = jnp.zeros((1, per_source), jnp.float32) + region.astype(jnp.float32)
    blank = jnp.zeros((1, per_source), jnp.float32)
    if per_source < LANES:
        meta_out_ref[...] = jnp.zeros_like(meta_out_ref)
    for h in range(patches):
        part = slice(h * per_source, (h + 1) * per_source)
        meta_out_ref[h, :, 0:per_source] = jnp.concatenate(
            [points[:, part], shares[:, part], here, blank], axis=0
        )

    def table(d):
        peer = lax.rem(region + d, patches)
        return pltpu.make_async_remote_copy(
            src_ref=meta_out_ref.at[peer],
            dst_ref=meta_in_ref.at[region],
            send_sem=ms_sem,
            recv_sem=mr_sem,
            device_id={"grid": peer},
            device_id_type=MESH,
        )

    local[2].wait()

    def block_of(q):
        return tall_ref.at[:, pl.ds(pl.multiple_of(q * coarse_dev, coarse_dev), coarse_dev)]

    rows = pairs // 10

    def narrow(i, carry):
        at = pl.ds(pl.multiple_of(i * rows, rows), rows)
        lanes = pl.ds(pl.multiple_of(region * coarse_dev, coarse_dev), coarse_dev)
        tall_ref[at, lanes] = t32_ref[at, :].astype(jnp.bfloat16)
        return carry

    lax.fori_loop(0, 10, narrow, 0)
    def along(way, s):
        block = block_of(region - 2 * way * s)
        return pltpu.make_async_remote_copy(
            src_ref=block,
            dst_ref=block,
            send_sem=ts_sem.at[(1 + way) // 2, s],
            recv_sem=tr_sem.at[(1 + way) // 2, s],
            device_id={"grid": region + 2 * way},
            device_id_type=MESH,
        )

    def across(at):
        block = block_of(2 * at + core)
        return pltpu.make_async_remote_copy(
            src_ref=block,
            dst_ref=block,
            send_sem=fs_sem,
            recv_sem=fr_sem,
            device_id={"grid": partner},
            device_id_type=MESH,
        )

    def has_next(way):
        return spot + 1 < spots if way == 1 else spot > 0

    def has_source(way, s):
        return spot >= s if way == 1 else spot + s < spots

    def relay(s):
        for way in (1, -1):

            @pl.when(has_source(way, s))
            def _(way=way):
                along(way, s - 1).wait_recv()

                @pl.when(has_next(way))
                def _():
                    along(way, s).start()

                across(spot - way * s).start()

    meet_grid()
    for d in range(1, patches):
        table(d).start()
    meta_in_ref[region] = meta_out_ref[region]

    for way in (1, -1):

        @pl.when(has_next(way))
        def _(way=way):
            along(way, 0).start()

    across(spot).start()

    arrived(meta_in_ref.at[1:], mr_sem)
    for gp in range(spots):
        meta_ref[me, gp] = meta_in_ref[2 * gp : 2 * gp + 2].reshape(16, LANES).astype(jnp.bfloat16)

    def tables(r):
        return pltpu.make_async_remote_copy(
            src_ref=meta_ref.at[me],
            dst_ref=meta_ref.at[me],
            send_sem=ns_sem,
            recv_sem=nr_sem,
            device_id={"member": member_peer(me, r, groups)},
            device_id_type=MESH,
        )

    for r in range(1, groups):
        tables(r).start()
    send_forecasts(early, chunks)

    def arrive(c):
        arrived(x_ref.at[c], xr_sem.at[c])

    def center(c):
        for lane in range(0, width, LANES):
            lanes = slice(lane, lane + LANES)

            def add(kk, total, lanes=lanes):
                for g in range(groups):
                    total = total + x_ref[c, g, kk, :, lanes].astype(jnp.float32)
                return total

            total = lax.fori_loop(0, mine, add, jnp.zeros((fields, LANES), jnp.float32))
            mean = total / members
            mean_ref[c, :, lanes] = mean

            def less(kk, carry, lanes=lanes, mean=mean):
                for g in range(groups):
                    d = x_ref[c, g, kk, :, lanes].astype(jnp.float32) - mean
                    dev_ref[c, g * mine + kk, :, lanes] = d.astype(jnp.bfloat16).astype(jnp.float32)
                return carry

            lax.fori_loop(0, mine, less, 0)

    def early_center(c, carry):
        arrive(c)
        center(c)
        return carry

    early_center(0, 0)
    for step_along in range(1, (spots + 1) // 2 + 1):
        relay(step_along)
    lax.fori_loop(1, early, early_center, 0)

    local[3].wait()
    arrived(meta_ref.at[1:], nr_sem)
    cells = lax.broadcasted_iota(jnp.int32, (columns, per_source), 0) + me * columns

    def look(gp, found):
        for m in range(groups):
            both = meta_ref[m, gp]
            if per_source < LANES:
                both = both[:, 0:per_source]
            for side in range(2):
                spots = mapping_ref[2 * gp + side, m : m + 1, :]
                onehot = jnp.where(cells == spots, 1.0, 0.0).astype(jnp.bfloat16)
                hit = lax.dot_general(
                    both, onehot, (((1,), (1,)), ((), ())), preferred_element_type=jnp.float32
                )
                found = found + hit[8 * side : 8 * side + 8]
        return found

    found = lax.fori_loop(0, spots, look, jnp.zeros((8, columns), jnp.float32))
    ids = found[0:3] + (found[6:7] * coarse_dev - RIM)
    ids = jnp.where(ids < 0.0, ids + coarse, ids)
    ids = jnp.where(ids >= coarse, ids - coarse, ids)
    for c in range(chunks):
        ids_ref[c, 0:3] = ids[:, c * width : (c + 1) * width]
        share_ref[c, 0:3] = found[3:6, c * width : (c + 1) * width]

    for step_along in range((spots + 1) // 2 + 1, spots):
        relay(step_along)
    arrived(tall_ref.at[:, 0 : spots * coarse_dev], fr_sem)

    def result(b, r):
        peer = member_peer(me, r, groups)
        at = pl.ds(pl.multiple_of(me * columns + b * LANES, LANES), LANES)
        return pltpu.make_async_remote_copy(
            src_ref=result_ref.at[b, pl.ds(peer * mine, mine)],
            dst_ref=out_hbm.at[:, :, at],
            send_sem=os_sem,
            recv_sem=or_sem,
            device_id={"member": peer},
            device_id_type=MESH,
        )

    def own_result(b):
        at = pl.ds(pl.multiple_of(me * columns + b * LANES, LANES), LANES)

        def put(kk, carry):
            out_hbm[kk, :, at] = result_ref[b, me * mine + kk]
            return carry

        lax.fori_loop(0, mine, put, 0)

    step = pairs // 4
    unroll = 8

    def update(c, carry):
        @pl.when(c >= early)
        def _():
            arrive(c)
            center(c)

        def place(q, z):
            at = pl.multiple_of(q * coarse_dev, coarse_dev)
            slots = lax.broadcasted_iota(jnp.int32, (coarse_dev, width), 0) + at
            slots = slots.astype(jnp.float32)
            spread = jnp.zeros((coarse_dev, width), jnp.float32)
            for s in range(3):
                hit = ids_ref[c, s : s + 1, :] == slots
                spread = spread + jnp.where(hit, share_ref[c, s : s + 1, :], 0.0)
            spread_ref[pl.ds(at, coarse_dev), :] = spread.astype(jnp.bfloat16)
            return z

        lax.fori_loop(0, patches, place, 0)

        def blend(i, z):
            at = pl.ds(pl.multiple_of(i * step, step), step)
            part = jnp.dot(tall_ref[at, :], spread_ref[...], preferred_element_type=jnp.float32)
            w_ref[pl.ds(i * (step // 8), step // 8)] = part.reshape(step // 8, 8, width)
            return z

        lax.fori_loop(0, 4, blend, 0)

        for lane in range(0, width, LANES):
            lanes = slice(lane, lane + LANES)
            b = c * (width // LANES) + lane // LANES

            def contract(jg, z, lanes=lanes, b=b):
                for first in (0, 4):

                    def some(kk, accs, first=first):
                        accs = list(accs)
                        for u in range(unroll):
                            k = kk * unroll + u
                            d = dev_ref[c, k, :, lanes]
                            for jj in range(4):
                                row = first + jj
                                w = w_ref[k * (members // 8) + jg, row : row + 1, lanes]
                                accs[jj] = accs[jj] + d * w
                        return tuple(accs)

                    start = tuple(mean_ref[c, :, lanes] for _ in range(4))
                    accs = lax.fori_loop(0, members // unroll, some, start)
                    for jj in range(4):
                        result_ref[b, jg * 8 + first + jj] = accs[jj].astype(jnp.bfloat16)
                return z

            lax.fori_loop(0, members // 8, contract, 0)
            for r in range(1, groups):
                result(b, r).start()
            own_result(b)
        return carry

    lax.fori_loop(0, chunks, update, 0)

    arrived(meta_in_ref.at[1:], ms_sem)
    arrived(meta_ref.at[1:], ns_sem)
    for s in range(spots - 1):
        for way in (1, -1):

            @pl.when(has_next(way) & has_source(way, s))
            def _(way=way, s=s):
                along(way, s).wait_send()

    arrived(tall_ref.at[:, 0 : spots * coarse_dev], fs_sem)
    others = x_ref.at[:, 1:]
    arrived(others, xs_sem)
    arrived(others, os_sem)
    arrived(others, or_sem)


def on_device(prior, mapping, triples, factors, transforms):
    groups = lax.axis_size("member")
    patches = lax.axis_size("grid")
    mine, fields, cells = prior.shape
    members = mine * groups
    columns = cells // groups
    per_source = mapping.shape[2]
    pairs, coarse_dev = transforms.shape
    coarse = coarse_dev * patches
    width = min(256, columns)
    chunks = columns // width
    blocks = columns // LANES
    anywhere = pl.BlockSpec(memory_space=pl.ANY)
    dma = pltpu.SemaphoreType.DMA
    return pl.pallas_call(
        functools.partial(exchange_kernel, groups, patches),
        out_shape=pltpu.VMEM(prior.shape, jnp.bfloat16),
        in_specs=[anywhere] * 5,
        out_specs=pl.BlockSpec(memory_space=pltpu.VMEM),
        scratch_shapes=[
            pltpu.VMEM((patches, groups, per_source), jnp.int32),
            pltpu.VMEM((3, columns), jnp.int32),
            pltpu.VMEM((3, columns), jnp.float32),
            pltpu.VMEM((pairs, coarse_dev), jnp.float32),
            pltpu.VMEM((pairs, coarse), jnp.bfloat16),
            pltpu.VMEM((patches, 8, LANES), jnp.float32),
            pltpu.VMEM((patches, 8, LANES), jnp.float32),
            pltpu.VMEM((groups, patches // 2, 16, LANES), jnp.bfloat16),
            pltpu.VMEM((chunks, 8, width), jnp.float32),
            pltpu.VMEM((chunks, 8, width), jnp.float32),
            pltpu.VMEM((chunks, groups, mine, fields, width), jnp.bfloat16),
            pltpu.VMEM((chunks, members, fields, width), jnp.float32),
            pltpu.VMEM((chunks, fields, width), jnp.float32),
            pltpu.VMEM((coarse, width), jnp.bfloat16),
            pltpu.VMEM((pairs // 8, 8, width), jnp.float32),
            pltpu.VMEM((blocks, members, fields, LANES), jnp.bfloat16),
            pltpu.VMEM((groups - 1, mine, fields, width), jnp.bfloat16),
            dma((4,)),
            dma,
            dma,
            dma((chunks,)),
            pltpu.SemaphoreType.REGULAR,
            pltpu.SemaphoreType.REGULAR,
            dma((2, patches // 2)),
            dma((2, patches // 2)),
            dma,
            dma,
            dma,
            dma,
            dma,
            dma,
            dma,
            dma,
        ],
        compiler_params=pltpu.CompilerParams(
            collective_id=0, has_side_effects=True, vmem_limit_bytes=44 * 1024 * 1024
        ),
        name="exchange",
    )(*[
        pltpu.with_memory_space_constraint(a, pltpu.HBM)
        for a in (
            mapping,
            jnp.transpose(triples, (1, 0, 2)),
            jnp.transpose(factors, (1, 0, 2)),
            transforms,
            prior,
        )
    ])


def solution(mesh):
    return jax.shard_map(
        on_device,
        mesh=mesh,
        in_specs=(
            P("member", None, "grid"),
            P(None, None, "grid"),
            P("grid", None, "member"),
            P("grid", None, "member"),
            P(None, "grid"),
        ),
        out_specs=P("member", None, "grid"),
        check_vma=False,
    )
```

```python
import functools

import jax
import jax.numpy as jnp
from jax import lax
from jax.experimental import pallas as pl
from jax.experimental.pallas import tpu as pltpu
from jax.sharding import PartitionSpec as P

RIM = 16
LANES = 128
HALVES = 2
MESH = pl.DeviceIdType.MESH


def member_peer(me, r, n):
    if n & (n - 1):
        return lax.rem(me + r, n)
    peer = me
    bit = 1
    while bit < n:
        if r & bit:
            peer = peer + bit * (1 - 2 * lax.rem(me // bit, 2))
        bit *= 2
    return peer


def exchange_kernel(
    groups,
    patches,
    mapping_hbm,
    triples_hbm,
    factors_hbm,
    transforms_hbm,
    prior_hbm,
    out_hbm,
    mapping_ref,
    triples_ref,
    factors_ref,
    t32_ref,
    tall_ref,
    meta_out_ref,
    meta_in_ref,
    meta_ref,
    ids_ref,
    share_ref,
    x_ref,
    dev_ref,
    mean_ref,
    spread_ref,
    w_ref,
    result_ref,
    stage_ref,
    local_sem,
    stage_sem,
    xs_sem,
    xr_sem,
    near_sem,
    far_sem,
    ts_sem,
    tr_sem,
    fs_sem,
    fr_sem,
    ms_sem,
    mr_sem,
    ns_sem,
    nr_sem,
    os_sem,
    or_sem,
):
    me = lax.axis_index("member")
    region = lax.axis_index("grid")
    chunks, _, mine, fields, width = x_ref.shape
    members = mine * groups
    columns = chunks * width
    pairs, coarse = tall_ref.shape
    coarse_dev = coarse // patches
    per_source = mapping_ref.shape[2]
    partner = region + 1 - 2 * lax.rem(region, 2)

    core = lax.rem(region, 2)
    spot = region // 2
    spots = patches // 2
    barrier = pltpu.get_barrier_semaphore()
    for r in range(groups):
        hub = {"member": member_peer(me, r, groups), "grid": 2 * spot + 1}
        if r:
            pl.semaphore_signal(barrier, inc=1, device_id=hub, device_id_type=MESH)
        else:

            @pl.when(core == 0)
            def _(hub=hub):
                pl.semaphore_signal(barrier, inc=1, device_id=hub, device_id_type=MESH)

    def meet_grid():
        @pl.when(core == 0)
        def _():
            pl.semaphore_wait(barrier, spots - 1)
            pl.semaphore_signal(far_sem, inc=1, device_id={"grid": partner}, device_id_type=MESH)

        @pl.when(core == 1)
        def _():
            pl.semaphore_wait(far_sem, 1)

    def forecast(c, r, staged=False):
        peer = member_peer(me, r, groups)
        at = pl.ds(pl.multiple_of(peer * columns + c * width, width), width)
        return pltpu.make_async_remote_copy(
            src_ref=stage_ref.at[r - 1] if staged else prior_hbm.at[:, :, at],
            dst_ref=x_ref.at[c, me],
            send_sem=xs_sem,
            recv_sem=xr_sem.at[c],
            device_id={"member": peer},
            device_id_type=MESH,
        )

    def send_forecasts(first, last):
        def some(c, carry):
            for r in range(1, groups):
                forecast(c, r).start()
            return carry

        lax.fori_loop(first, last, some, 0)

    def arrived(ref, sem):
        pltpu.make_async_copy(ref, ref, sem).wait()

    early = (chunks + 1) // 2
    for r in range(1, groups):
        at = pl.ds(pl.multiple_of(member_peer(me, r, groups) * columns, width), width)
        pltpu.make_async_copy(prior_hbm.at[:, :, at], stage_ref.at[r - 1], stage_sem).start()
    local = [
        pltpu.make_async_copy(triples_hbm.at[:, 0], triples_ref, local_sem.at[0]),
        pltpu.make_async_copy(factors_hbm.at[:, 0], factors_ref, local_sem.at[1]),
        pltpu.make_async_copy(transforms_hbm, t32_ref, local_sem.at[2]),
        pltpu.make_async_copy(mapping_hbm, mapping_ref, local_sem.at[3]),
    ]
    for copy in local:
        copy.start()
    arrived(stage_ref, stage_sem)

    @pl.when(core == 1)
    def _():
        pl.semaphore_wait(barrier, 2 * groups - 1)
        pl.semaphore_signal(near_sem, inc=1, device_id={"grid": partner}, device_id_type=MESH)

    @pl.when(core == 0)
    def _():
        pl.semaphore_wait(near_sem, 1)
        for d in range(1, spots):
            other = 2 * lax.rem(spot + d, spots)
            pl.semaphore_signal(barrier, inc=1, device_id={"grid": other}, device_id_type=MESH)

    for r in range(1, groups):
        forecast(0, r, True).start()
    send_forecasts(1, early)

    def own_forecast(c, carry):
        at = pl.ds(pl.multiple_of(me * columns + c * width, width), width)
        pltpu.make_async_copy(prior_hbm.at[:, :, at], x_ref.at[c, me], xr_sem.at[c]).start()
        return carry

    lax.fori_loop(0, chunks, own_forecast, 0)

    local[0].wait()
    local[1].wait()
    raw = factors_ref[...]
    shares = raw / jnp.sum(raw, axis=0, keepdims=True)
    points = triples_ref[...].astype(jnp.float32) + 1.0
    blank = jnp.zeros((2, per_source), jnp.float32)
    if per_source < LANES:
        meta_out_ref[...] = jnp.zeros_like(meta_out_ref)
    for h in range(patches):
        part = slice(h * per_source, (h + 1) * per_source)
        meta_out_ref[h, :, 0:per_source] = jnp.concatenate(
            [points[:, part], shares[:, part], blank], axis=0
        )

    def table(d):
        peer = lax.rem(region + d, patches)
        return pltpu.make_async_remote_copy(
            src_ref=meta_out_ref.at[peer],
            dst_ref=meta_in_ref.at[region],
            send_sem=ms_sem,
            recv_sem=mr_sem,
            device_id={"grid": peer},
            device_id_type=MESH,
        )

    local[2].wait()

    def block_of(q, part):
        rows = pairs // HALVES
        lanes = pl.ds(pl.multiple_of(q * coarse_dev, coarse_dev), coarse_dev)
        return tall_ref.at[part * rows : (part + 1) * rows, lanes]

    rows = pairs // 10

    def narrow(i, carry):
        at = pl.ds(pl.multiple_of(i * rows, rows), rows)
        lanes = pl.ds(pl.multiple_of(region * coarse_dev, coarse_dev), coarse_dev)
        tall_ref[at, lanes] = t32_ref[at, :].astype(jnp.bfloat16)
        return carry

    lax.fori_loop(0, 10, narrow, 0)
    def along(way, s, part):
        block = block_of(region - 2 * way * s, part)
        return pltpu.make_async_remote_copy(
            src_ref=block,
            dst_ref=block,
            send_sem=ts_sem.at[(1 + way) // 2],
            recv_sem=tr_sem.at[(1 + way) // 2, s, part],
            device_id={"grid": region + 2 * way},
            device_id_type=MESH,
        )

    def across(at, part):
        block = block_of(2 * at + core, part)
        return pltpu.make_async_remote_copy(
            src_ref=block,
            dst_ref=block,
            send_sem=fs_sem,
            recv_sem=fr_sem,
            device_id={"grid": partner},
            device_id_type=MESH,
        )

    def has_next(way):
        return spot + 1 < spots if way == 1 else spot > 0

    def has_source(way, s):
        return spot >= s if way == 1 else spot + s < spots

    def relay(s, part):
        for way in (1, -1):

            @pl.when(has_source(way, s))
            def _(way=way):
                along(way, s - 1, part).wait_recv()

                @pl.when(has_next(way))
                def _():
                    along(way, s, part).start()

                across(spot - way * s, part).start()

    meet_grid()
    for d in range(1, patches):
        table(d).start()
    meta_in_ref[region] = meta_out_ref[region]

    for way in (1, -1):

        @pl.when(has_next(way))
        def _(way=way):
            for part in range(HALVES):
                along(way, 0, part).start()

    for part in range(HALVES):
        across(spot, part).start()

    arrived(meta_in_ref.at[1:], mr_sem)
    for first in range(0, patches, 8):
        packed = jnp.concatenate([meta_in_ref[first + u, 0:6] for u in range(8)], axis=0)
        meta_ref[me, first // 8] = packed.astype(jnp.bfloat16)

    def tables(r):
        return pltpu.make_async_remote_copy(
            src_ref=meta_ref.at[me],
            dst_ref=meta_ref.at[me],
            send_sem=ns_sem,
            recv_sem=nr_sem,
            device_id={"member": member_peer(me, r, groups)},
            device_id_type=MESH,
        )

    for r in range(1, groups):
        tables(r).start()
    send_forecasts(early, chunks)

    def arrive(c):
        arrived(x_ref.at[c], xr_sem.at[c])

    def center(c):
        for lane in range(0, width, LANES):
            lanes = slice(lane, lane + LANES)

            def add(kk, total, lanes=lanes):
                for g in range(groups):
                    total = total + x_ref[c, g, kk, :, lanes].astype(jnp.float32)
                return total

            total = lax.fori_loop(0, mine, add, jnp.zeros((fields, LANES), jnp.float32))
            mean = total / members
            mean_ref[c, :, lanes] = mean

            def less(kk, carry, lanes=lanes, mean=mean):
                for g in range(groups):
                    d = x_ref[c, g, kk, :, lanes].astype(jnp.float32) - mean
                    dev_ref[c, g * mine + kk, :, lanes] = d.astype(jnp.bfloat16).astype(jnp.float32)
                return carry

            lax.fori_loop(0, mine, less, 0)

    def early_center(c, carry):
        arrive(c)
        center(c)
        return carry

    hops = [(s, part) for s in range(1, spots) for part in range(HALVES)]
    middle = HALVES * ((spots + 1) // 2)
    for hop in hops[:1]:
        relay(*hop)
    early_center(0, 0)
    for hop in hops[1:middle]:
        relay(*hop)
    lax.fori_loop(1, early, early_center, 0)

    local[3].wait()
    arrived(meta_ref.at[1:], nr_sem)
    cells = lax.broadcasted_iota(jnp.int32, (columns, per_source), 0) + me * columns

    def look(octet, found):
        ids, shares = found
        for m in range(groups):
            packed = meta_ref[m, octet]
            if per_source < LANES:
                packed = packed[:, 0:per_source]
            for u in range(8):
                source = 8 * octet + u
                onehot = jnp.where(cells == mapping_ref[source, m : m + 1, :], 1.0, 0.0)
                hit = lax.dot_general(
                    packed,
                    onehot.astype(jnp.bfloat16),
                    (((1,), (1,)), ((), ())),
                    preferred_element_type=jnp.float32,
                )[6 * u : 6 * u + 6]
                base = (jnp.int32(source * coarse_dev) - (RIM + 1)).astype(jnp.float32)
                ids = ids + jnp.where(hit[0:1] > 0.5, hit[0:3] + base, 0.0)
                shares = shares + hit[3:6]
        return ids, shares

    nothing = jnp.zeros((3, columns), jnp.float32)
    ids, shares = lax.fori_loop(0, patches // 8, look, (nothing, nothing))
    ids = jnp.where(ids < 0.0, ids + coarse, ids)
    ids = jnp.where(ids >= coarse, ids - coarse, ids)
    for c in range(chunks):
        ids_ref[c, 0:3] = ids[:, c * width : (c + 1) * width]
        share_ref[c, 0:3] = shares[:, c * width : (c + 1) * width]

    for hop in hops[middle:]:
        relay(*hop)
    arrived(tall_ref.at[:, 0 : spots * coarse_dev], fr_sem)

    def result(b, r):
        peer = member_peer(me, r, groups)
        at = pl.ds(pl.multiple_of(me * columns + b * LANES, LANES), LANES)
        return pltpu.make_async_remote_copy(
            src_ref=result_ref.at[b, pl.ds(peer * mine, mine)],
            dst_ref=out_hbm.at[:, :, at],
            send_sem=os_sem,
            recv_sem=or_sem,
            device_id={"member": peer},
            device_id_type=MESH,
        )

    def own_result(b):
        at = pl.ds(pl.multiple_of(me * columns + b * LANES, LANES), LANES)

        def put(kk, carry):
            out_hbm[kk, :, at] = result_ref[b, me * mine + kk]
            return carry

        lax.fori_loop(0, mine, put, 0)

    step = pairs // 4
    unroll = 8

    def update(c, carry):
        @pl.when(c >= early)
        def _():
            arrive(c)
            center(c)

        def place(q, z):
            at = pl.multiple_of(q * coarse_dev, coarse_dev)
            slots = lax.broadcasted_iota(jnp.int32, (coarse_dev, width), 0) + at
            slots = slots.astype(jnp.float32)
            spread = jnp.zeros((coarse_dev, width), jnp.float32)
            for s in range(3):
                hit = ids_ref[c, s : s + 1, :] == slots
                spread = spread + jnp.where(hit, share_ref[c, s : s + 1, :], 0.0)
            spread_ref[pl.ds(at, coarse_dev), :] = spread.astype(jnp.bfloat16)
            return z

        lax.fori_loop(0, patches, place, 0)

        def blend(i, z):
            at = pl.ds(pl.multiple_of(i * step, step), step)
            part = jnp.dot(tall_ref[at, :], spread_ref[...], preferred_element_type=jnp.float32)
            w_ref[pl.ds(i * (step // 8), step // 8)] = part.reshape(step // 8, 8, width)
            return z

        lax.fori_loop(0, 4, blend, 0)

        for lane in range(0, width, LANES):
            lanes = slice(lane, lane + LANES)
            b = c * (width // LANES) + lane // LANES

            def contract(jg, z, lanes=lanes, b=b):
                for first in (0, 4):

                    def some(kk, accs, first=first):
                        accs = list(accs)
                        for u in range(unroll):
                            k = kk * unroll + u
                            d = dev_ref[c, k, :, lanes]
                            for jj in range(4):
                                row = first + jj
                                w = w_ref[k * (members // 8) + jg, row : row + 1, lanes]
                                accs[jj] = accs[jj] + d * w
                        return tuple(accs)

                    start = tuple(mean_ref[c, :, lanes] for _ in range(4))
                    accs = lax.fori_loop(0, members // unroll, some, start)
                    for jj in range(4):
                        result_ref[b, jg * 8 + first + jj] = accs[jj].astype(jnp.bfloat16)
                return z

            lax.fori_loop(0, members // 8, contract, 0)
            for r in range(1, groups):
                result(b, r).start()
            own_result(b)
        return carry

    lax.fori_loop(0, chunks, update, 0)

    arrived(meta_in_ref.at[1:], ms_sem)
    arrived(meta_ref.at[1:], ns_sem)
    for n in range(1, spots):
        for side, mark in ((1, n - 1), (0, spots - n)):

            @pl.when(spot == mark)
            def _(n=n, side=side):
                arrived(tall_ref.at[:, 0 : n * coarse_dev], ts_sem.at[side])

    arrived(tall_ref.at[:, 0 : spots * coarse_dev], fs_sem)
    others = x_ref.at[:, 1:]
    arrived(others, xs_sem)
    arrived(others, os_sem)
    arrived(others, or_sem)


def on_device(prior, mapping, triples, factors, transforms):
    groups = lax.axis_size("member")
    patches = lax.axis_size("grid")
    mine, fields, cells = prior.shape
    members = mine * groups
    columns = cells // groups
    per_source = mapping.shape[2]
    pairs, coarse_dev = transforms.shape
    coarse = coarse_dev * patches
    width = min(256, columns)
    chunks = columns // width
    blocks = columns // LANES
    anywhere = pl.BlockSpec(memory_space=pl.ANY)
    dma = pltpu.SemaphoreType.DMA
    return pl.pallas_call(
        functools.partial(exchange_kernel, groups, patches),
        out_shape=pltpu.VMEM(prior.shape, jnp.bfloat16),
        in_specs=[anywhere] * 5,
        out_specs=pl.BlockSpec(memory_space=pltpu.VMEM),
        scratch_shapes=[
            pltpu.VMEM((patches, groups, per_source), jnp.int32),
            pltpu.VMEM((3, columns), jnp.int32),
            pltpu.VMEM((3, columns), jnp.float32),
            pltpu.VMEM((pairs, coarse_dev), jnp.float32),
            pltpu.VMEM((pairs, coarse), jnp.bfloat16),
            pltpu.VMEM((patches, 8, LANES), jnp.float32),
            pltpu.VMEM((patches, 8, LANES), jnp.float32),
            pltpu.VMEM((groups, patches // 8, 48, LANES), jnp.bfloat16),
            pltpu.VMEM((chunks, 8, width), jnp.float32),
            pltpu.VMEM((chunks, 8, width), jnp.float32),
            pltpu.VMEM((chunks, groups, mine, fields, width), jnp.bfloat16),
            pltpu.VMEM((chunks, members, fields, width), jnp.float32),
            pltpu.VMEM((chunks, fields, width), jnp.float32),
            pltpu.VMEM((coarse, width), jnp.bfloat16),
            pltpu.VMEM((pairs // 8, 8, width), jnp.float32),
            pltpu.VMEM((blocks, members, fields, LANES), jnp.bfloat16),
            pltpu.VMEM((groups - 1, mine, fields, width), jnp.bfloat16),
            dma((4,)),
            dma,
            dma,
            dma((chunks,)),
            pltpu.SemaphoreType.REGULAR,
            pltpu.SemaphoreType.REGULAR,
            dma((2,)),
            dma((2, patches // 2 - 1, HALVES)),
            dma,
            dma,
            dma,
            dma,
            dma,
            dma,
            dma,
            dma,
        ],
        compiler_params=pltpu.CompilerParams(
            collective_id=0, has_side_effects=True, vmem_limit_bytes=44 * 1024 * 1024
        ),
        name="exchange",
    )(*[
        pltpu.with_memory_space_constraint(a, pltpu.HBM)
        for a in (
            mapping,
            jnp.transpose(triples, (1, 0, 2)),
            jnp.transpose(factors, (1, 0, 2)),
            transforms,
            prior,
        )
    ])


def solution(mesh):
    return jax.shard_map(
        on_device,
        mesh=mesh,
        in_specs=(
            P("member", None, "grid"),
            P(None, None, "grid"),
            P("grid", None, "member"),
            P("grid", None, "member"),
            P(None, "grid"),
        ),
        out_specs=P("member", None, "grid"),
        check_vma=False,
    )
```

```python
import functools

import jax
import jax.numpy as jnp
from jax import lax
from jax.experimental import pallas as pl
from jax.experimental.pallas import tpu as pltpu
from jax.sharding import PartitionSpec as P

RIM = 16
LANES = 128
HALVES = 2
MESH = pl.DeviceIdType.MESH


def member_peer(me, r, n):
    if n & (n - 1):
        return lax.rem(me + r, n)
    peer = me
    bit = 1
    while bit < n:
        if r & bit:
            peer = peer + bit * (1 - 2 * lax.rem(me // bit, 2))
        bit *= 2
    return peer


def exchange_kernel(
    groups,
    patches,
    mapping_hbm,
    triples_hbm,
    factors_hbm,
    transforms_hbm,
    prior_hbm,
    out_hbm,
    mapping_ref,
    triples_ref,
    factors_ref,
    t32_ref,
    tall_ref,
    meta_out_ref,
    meta_in_ref,
    meta_ref,
    ids_ref,
    share_ref,
    x_ref,
    dev_ref,
    mean_ref,
    spread_ref,
    w_ref,
    result_ref,
    stage_ref,
    local_sem,
    stage_sem,
    xs_sem,
    xr_sem,
    near_sem,
    far_sem,
    ts_sem,
    tr_sem,
    fs_sem,
    fr_sem,
    ms_sem,
    mr_sem,
    ns_sem,
    nr_sem,
    os_sem,
    or_sem,
):
    me = lax.axis_index("member")
    region = lax.axis_index("grid")
    chunks, _, mine, fields, width = x_ref.shape
    members = mine * groups
    columns = chunks * width
    pairs, coarse = tall_ref.shape
    coarse_dev = coarse // patches
    per_source = mapping_ref.shape[2]
    partner = region + 1 - 2 * lax.rem(region, 2)

    core = lax.rem(region, 2)
    spot = region // 2
    spots = patches // 2
    barrier = pltpu.get_barrier_semaphore()
    for r in range(groups):
        hub = {"member": member_peer(me, r, groups), "grid": 2 * spot + 1}
        if r:
            pl.semaphore_signal(barrier, inc=1, device_id=hub, device_id_type=MESH)
        else:

            @pl.when(core == 0)
            def _(hub=hub):
                pl.semaphore_signal(barrier, inc=1, device_id=hub, device_id_type=MESH)

    def meet_grid():
        @pl.when(core == 0)
        def _():
            pl.semaphore_wait(barrier, spots - 1)
            pl.semaphore_signal(far_sem, inc=1, device_id={"grid": partner}, device_id_type=MESH)

        @pl.when(core == 1)
        def _():
            pl.semaphore_wait(far_sem, 1)

    def forecast(c, r, staged=0):
        peer = member_peer(me, r, groups)
        at = pl.ds(pl.multiple_of(peer * columns + c * width, width), width)
        if staged == 1:
            at = pl.ds(pl.multiple_of(peer * columns + LANES, LANES), width - LANES)
        source = stage_ref.at[r - 1] if staged == 2 else prior_hbm.at[:, :, at]
        target = x_ref.at[c, me]
        if staged:
            target = target.at[:, :, LANES:] if staged == 1 else target.at[:, :, 0:LANES]
        return pltpu.make_async_remote_copy(
            src_ref=source,
            dst_ref=target,
            send_sem=xs_sem,
            recv_sem=xr_sem.at[c],
            device_id={"member": peer},
            device_id_type=MESH,
        )

    def send_forecasts(first, last):
        def some(c, carry):
            for r in range(1, groups):
                forecast(c, r).start()
            return carry

        lax.fori_loop(first, last, some, 0)

    def arrived(ref, sem):
        pltpu.make_async_copy(ref, ref, sem).wait()

    early = (chunks + 1) // 2
    for r in range(1, groups):
        at = pl.ds(pl.multiple_of(member_peer(me, r, groups) * columns, LANES), LANES)
        pltpu.make_async_copy(prior_hbm.at[:, :, at], stage_ref.at[r - 1], stage_sem).start()
    local = [
        pltpu.make_async_copy(triples_hbm.at[:, 0], triples_ref, local_sem.at[0]),
        pltpu.make_async_copy(factors_hbm.at[:, 0], factors_ref, local_sem.at[1]),
        pltpu.make_async_copy(transforms_hbm, t32_ref, local_sem.at[2]),
        pltpu.make_async_copy(mapping_hbm, mapping_ref, local_sem.at[3]),
    ]
    for copy in local:
        copy.start()
    arrived(stage_ref, stage_sem)

    @pl.when(core == 1)
    def _():
        pl.semaphore_wait(barrier, 2 * groups - 1)
        pl.semaphore_signal(near_sem, inc=1, device_id={"grid": partner}, device_id_type=MESH)

    @pl.when(core == 0)
    def _():
        pl.semaphore_wait(near_sem, 1)
        for d in range(1, spots):
            other = 2 * lax.rem(spot + d, spots)
            pl.semaphore_signal(barrier, inc=1, device_id={"grid": other}, device_id_type=MESH)

    for staged in (2, 1):
        for r in range(1, groups):
            forecast(0, r, staged).start()
    send_forecasts(1, early)

    def own_forecast(c, carry):
        at = pl.ds(pl.multiple_of(me * columns + c * width, width), width)
        pltpu.make_async_copy(prior_hbm.at[:, :, at], x_ref.at[c, me], xr_sem.at[c]).start()
        return carry

    lax.fori_loop(0, chunks, own_forecast, 0)

    local[0].wait()
    local[1].wait()
    raw = factors_ref[...]
    shares = raw / jnp.sum(raw, axis=0, keepdims=True)
    points = triples_ref[...].astype(jnp.float32) + 1.0
    blank = jnp.zeros((2, per_source), jnp.float32)
    if per_source < LANES:
        meta_out_ref[...] = jnp.zeros_like(meta_out_ref)
    for h in range(patches):
        part = slice(h * per_source, (h + 1) * per_source)
        meta_out_ref[h, :, 0:per_source] = jnp.concatenate(
            [points[:, part], shares[:, part], blank], axis=0
        )

    def table(d):
        peer = lax.rem(region + d, patches)
        return pltpu.make_async_remote_copy(
            src_ref=meta_out_ref.at[peer],
            dst_ref=meta_in_ref.at[region],
            send_sem=ms_sem,
            recv_sem=mr_sem,
            device_id={"grid": peer},
            device_id_type=MESH,
        )

    local[2].wait()

    def block_of(q, part):
        rows = pairs // HALVES
        lanes = pl.ds(pl.multiple_of(q * coarse_dev, coarse_dev), coarse_dev)
        return tall_ref.at[part * rows : (part + 1) * rows, lanes]

    rows = pairs // 10

    def narrow(i, carry):
        at = pl.ds(pl.multiple_of(i * rows, rows), rows)
        lanes = pl.ds(pl.multiple_of(region * coarse_dev, coarse_dev), coarse_dev)
        tall_ref[at, lanes] = t32_ref[at, :].astype(jnp.bfloat16)
        return carry

    lax.fori_loop(0, 10, narrow, 0)
    def along(way, s, part):
        block = block_of(region - 2 * way * s, part)
        return pltpu.make_async_remote_copy(
            src_ref=block,
            dst_ref=block,
            send_sem=ts_sem.at[(1 + way) // 2],
            recv_sem=tr_sem.at[(1 + way) // 2, s, part],
            device_id={"grid": region + 2 * way},
            device_id_type=MESH,
        )

    def across(at, part):
        block = block_of(2 * at + core, part)
        return pltpu.make_async_remote_copy(
            src_ref=block,
            dst_ref=block,
            send_sem=fs_sem,
            recv_sem=fr_sem,
            device_id={"grid": partner},
            device_id_type=MESH,
        )

    def has_next(way):
        return spot + 1 < spots if way == 1 else spot > 0

    def has_source(way, s):
        return spot >= s if way == 1 else spot + s < spots

    def relay(s, part):
        for way in (1, -1):

            @pl.when(has_source(way, s))
            def _(way=way):
                along(way, s - 1, part).wait_recv()

                @pl.when(has_next(way))
                def _():
                    along(way, s, part).start()

                across(spot - way * s, part).start()

    meet_grid()
    for d in range(1, patches):
        table(d).start()
    meta_in_ref[region] = meta_out_ref[region]

    for way in (1, -1):

        @pl.when(has_next(way))
        def _(way=way):
            for part in range(HALVES):
                along(way, 0, part).start()

    for part in range(HALVES):
        across(spot, part).start()

    arrived(meta_in_ref.at[1:], mr_sem)
    for first in range(0, patches, 8):
        packed = jnp.concatenate([meta_in_ref[first + u, 0:6] for u in range(8)], axis=0)
        meta_ref[me, first // 8] = packed.astype(jnp.bfloat16)

    def tables(r):
        return pltpu.make_async_remote_copy(
            src_ref=meta_ref.at[me],
            dst_ref=meta_ref.at[me],
            send_sem=ns_sem,
            recv_sem=nr_sem,
            device_id={"member": member_peer(me, r, groups)},
            device_id_type=MESH,
        )

    for r in range(1, groups):
        tables(r).start()
    send_forecasts(early, chunks)

    def arrive(c):
        arrived(x_ref.at[c], xr_sem.at[c])

    def center(c):
        for lane in range(0, width, LANES):
            lanes = slice(lane, lane + LANES)

            def add(kk, total, lanes=lanes):
                for g in range(groups):
                    total = total + x_ref[c, g, kk, :, lanes].astype(jnp.float32)
                return total

            total = lax.fori_loop(0, mine, add, jnp.zeros((fields, LANES), jnp.float32))
            mean = total / members
            mean_ref[c, :, lanes] = mean

            def less(kk, carry, lanes=lanes, mean=mean):
                for g in range(groups):
                    d = x_ref[c, g, kk, :, lanes].astype(jnp.float32) - mean
                    dev_ref[c, g * mine + kk, :, lanes] = d.astype(jnp.bfloat16).astype(jnp.float32)
                return carry

            lax.fori_loop(0, mine, less, 0)

    def early_center(c, carry):
        arrive(c)
        center(c)
        return carry

    hops = [(s, part) for s in range(1, spots) for part in range(HALVES)]
    middle = HALVES * ((spots + 1) // 2)
    for hop in hops[:1]:
        relay(*hop)
    early_center(0, 0)
    for hop in hops[1:middle]:
        relay(*hop)
    lax.fori_loop(1, early, early_center, 0)

    local[3].wait()
    arrived(meta_ref.at[1:], nr_sem)
    cells = lax.broadcasted_iota(jnp.int32, (columns, per_source), 0) + me * columns

    def look(octet, found):
        ids, shares = found
        for m in range(groups):
            packed = meta_ref[m, octet]
            if per_source < LANES:
                packed = packed[:, 0:per_source]
            for u in range(8):
                source = 8 * octet + u
                onehot = jnp.where(cells == mapping_ref[source, m : m + 1, :], 1.0, 0.0)
                hit = lax.dot_general(
                    packed,
                    onehot.astype(jnp.bfloat16),
                    (((1,), (1,)), ((), ())),
                    preferred_element_type=jnp.float32,
                )[6 * u : 6 * u + 6]
                base = (jnp.int32(source * coarse_dev) - (RIM + 1)).astype(jnp.float32)
                ids = ids + jnp.where(hit[0:1] > 0.5, hit[0:3] + base, 0.0)
                shares = shares + hit[3:6]
        return ids, shares

    nothing = jnp.zeros((3, columns), jnp.float32)
    ids, shares = lax.fori_loop(0, patches // 8, look, (nothing, nothing))
    ids = jnp.where(ids < 0.0, ids + coarse, ids)
    ids = jnp.where(ids >= coarse, ids - coarse, ids)
    for c in range(chunks):
        ids_ref[c, 0:3] = ids[:, c * width : (c + 1) * width]
        share_ref[c, 0:3] = shares[:, c * width : (c + 1) * width]

    for hop in hops[middle:]:
        relay(*hop)
    arrived(tall_ref.at[:, 0 : spots * coarse_dev], fr_sem)

    def result(b, r):
        peer = member_peer(me, r, groups)
        at = pl.ds(pl.multiple_of(me * columns + b * LANES, LANES), LANES)
        return pltpu.make_async_remote_copy(
            src_ref=result_ref.at[b, pl.ds(peer * mine, mine)],
            dst_ref=out_hbm.at[:, :, at],
            send_sem=os_sem,
            recv_sem=or_sem,
            device_id={"member": peer},
            device_id_type=MESH,
        )

    def own_result(b):
        at = pl.ds(pl.multiple_of(me * columns + b * LANES, LANES), LANES)

        def put(kk, carry):
            out_hbm[kk, :, at] = result_ref[b, me * mine + kk]
            return carry

        lax.fori_loop(0, mine, put, 0)

    step = pairs // 4
    unroll = 8

    def update(c, carry):
        @pl.when(c >= early)
        def _():
            arrive(c)
            center(c)

        def place(q, z):
            at = pl.multiple_of(q * coarse_dev, coarse_dev)
            slots = lax.broadcasted_iota(jnp.int32, (coarse_dev, width), 0) + at
            slots = slots.astype(jnp.float32)
            spread = jnp.zeros((coarse_dev, width), jnp.float32)
            for s in range(3):
                hit = ids_ref[c, s : s + 1, :] == slots
                spread = spread + jnp.where(hit, share_ref[c, s : s + 1, :], 0.0)
            spread_ref[pl.ds(at, coarse_dev), :] = spread.astype(jnp.bfloat16)
            return z

        lax.fori_loop(0, patches, place, 0)

        def blend(i, z):
            at = pl.ds(pl.multiple_of(i * step, step), step)
            part = jnp.dot(tall_ref[at, :], spread_ref[...], preferred_element_type=jnp.float32)
            w_ref[pl.ds(i * (step // 8), step // 8)] = part.reshape(step // 8, 8, width)
            return z

        lax.fori_loop(0, 4, blend, 0)

        for lane in range(0, width, LANES):
            lanes = slice(lane, lane + LANES)
            b = c * (width // LANES) + lane // LANES

            def contract(jg, z, lanes=lanes, b=b):
                for first in (0, 4):

                    def some(kk, accs, first=first):
                        accs = list(accs)
                        for u in range(unroll):
                            k = kk * unroll + u
                            d = dev_ref[c, k, :, lanes]
                            for jj in range(4):
                                row = first + jj
                                w = w_ref[k * (members // 8) + jg, row : row + 1, lanes]
                                accs[jj] = accs[jj] + d * w
                        return tuple(accs)

                    start = tuple(mean_ref[c, :, lanes] for _ in range(4))
                    accs = lax.fori_loop(0, members // unroll, some, start)
                    for jj in range(4):
                        result_ref[b, jg * 8 + first + jj] = accs[jj].astype(jnp.bfloat16)
                return z

            lax.fori_loop(0, members // 8, contract, 0)
            for r in range(1, groups):
                result(b, r).start()
            own_result(b)
        return carry

    lax.fori_loop(0, chunks, update, 0)

    arrived(meta_in_ref.at[1:], ms_sem)
    arrived(meta_ref.at[1:], ns_sem)
    for n in range(1, spots):
        for side, mark in ((1, n - 1), (0, spots - n)):

            @pl.when(spot == mark)
            def _(n=n, side=side):
                arrived(tall_ref.at[:, 0 : n * coarse_dev], ts_sem.at[side])

    arrived(tall_ref.at[:, 0 : spots * coarse_dev], fs_sem)
    others = x_ref.at[:, 1:]
    arrived(others, xs_sem)
    arrived(others, os_sem)
    arrived(others, or_sem)


def on_device(prior, mapping, triples, factors, transforms):
    groups = lax.axis_size("member")
    patches = lax.axis_size("grid")
    mine, fields, cells = prior.shape
    members = mine * groups
    columns = cells // groups
    per_source = mapping.shape[2]
    pairs, coarse_dev = transforms.shape
    coarse = coarse_dev * patches
    width = min(256, columns)
    chunks = columns // width
    blocks = columns // LANES
    anywhere = pl.BlockSpec(memory_space=pl.ANY)
    dma = pltpu.SemaphoreType.DMA
    return pl.pallas_call(
        functools.partial(exchange_kernel, groups, patches),
        out_shape=pltpu.VMEM(prior.shape, jnp.bfloat16),
        in_specs=[anywhere] * 5,
        out_specs=pl.BlockSpec(memory_space=pltpu.VMEM),
        scratch_shapes=[
            pltpu.VMEM((patches, groups, per_source), jnp.int32),
            pltpu.VMEM((3, columns), jnp.int32),
            pltpu.VMEM((3, columns), jnp.float32),
            pltpu.VMEM((pairs, coarse_dev), jnp.float32),
            pltpu.VMEM((pairs, coarse), jnp.bfloat16),
            pltpu.VMEM((patches, 8, LANES), jnp.float32),
            pltpu.VMEM((patches, 8, LANES), jnp.float32),
            pltpu.VMEM((groups, patches // 8, 48, LANES), jnp.bfloat16),
            pltpu.VMEM((chunks, 8, width), jnp.float32),
            pltpu.VMEM((chunks, 8, width), jnp.float32),
            pltpu.VMEM((chunks, groups, mine, fields, width), jnp.bfloat16),
            pltpu.VMEM((chunks, members, fields, width), jnp.float32),
            pltpu.VMEM((chunks, fields, width), jnp.float32),
            pltpu.VMEM((coarse, width), jnp.bfloat16),
            pltpu.VMEM((pairs // 8, 8, width), jnp.float32),
            pltpu.VMEM((blocks, members, fields, LANES), jnp.bfloat16),
            pltpu.VMEM((groups - 1, mine, fields, LANES), jnp.bfloat16),
            dma((4,)),
            dma,
            dma,
            dma((chunks,)),
            pltpu.SemaphoreType.REGULAR,
            pltpu.SemaphoreType.REGULAR,
            dma((2,)),
            dma((2, patches // 2 - 1, HALVES)),
            dma,
            dma,
            dma,
            dma,
            dma,
            dma,
            dma,
            dma,
        ],
        compiler_params=pltpu.CompilerParams(
            collective_id=0, has_side_effects=True, vmem_limit_bytes=44 * 1024 * 1024
        ),
        name="exchange",
    )(*[
        pltpu.with_memory_space_constraint(a, pltpu.HBM)
        for a in (
            mapping,
            jnp.transpose(triples, (1, 0, 2)),
            jnp.transpose(factors, (1, 0, 2)),
            transforms,
            prior,
        )
    ])


def solution(mesh):
    return jax.shard_map(
        on_device,
        mesh=mesh,
        in_specs=(
            P("member", None, "grid"),
            P(None, None, "grid"),
            P("grid", None, "member"),
            P("grid", None, "member"),
            P(None, "grid"),
        ),
        out_specs=P("member", None, "grid"),
        check_vma=False,
    )
```

```python
import functools

import jax
import jax.numpy as jnp
from jax import lax
from jax.experimental import pallas as pl
from jax.experimental.pallas import tpu as pltpu
from jax.sharding import PartitionSpec as P

RIM = 16
LANES = 128
HALVES = 2
MESH = pl.DeviceIdType.MESH


def member_peer(me, r, n):
    if n & (n - 1):
        return lax.rem(me + r, n)
    peer = me
    bit = 1
    while bit < n:
        if r & bit:
            peer = peer + bit * (1 - 2 * lax.rem(me // bit, 2))
        bit *= 2
    return peer


def split_peers(n):
    others = range(1, n)
    if n & (n - 1):
        return list(others), []
    return [r for r in others if not r & (r - 1)], [r for r in others if r & (r - 1)]


def exchange_kernel(
    groups,
    patches,
    mapping_hbm,
    triples_hbm,
    factors_hbm,
    transforms_hbm,
    prior_hbm,
    out_hbm,
    mapping_ref,
    triples_ref,
    factors_ref,
    t32_ref,
    tall_ref,
    meta_out_ref,
    meta_in_ref,
    meta_ref,
    ids_ref,
    share_ref,
    x_ref,
    dev_ref,
    mean_ref,
    spread_ref,
    w_ref,
    result_ref,
    stage_ref,
    local_sem,
    stage_sem,
    xs_sem,
    xr_sem,
    near_sem,
    all_sem,
    far_sem,
    hub_sem,
    ts_sem,
    tr_sem,
    fs_sem,
    fr_sem,
    ms_sem,
    mr_sem,
    ns_sem,
    nr_sem,
    os_sem,
    or_sem,
):
    me = lax.axis_index("member")
    region = lax.axis_index("grid")
    chunks, _, mine, fields, width = x_ref.shape
    members = mine * groups
    columns = chunks * width
    pairs, coarse = tall_ref.shape
    coarse_dev = coarse // patches
    per_source = mapping_ref.shape[2]
    partner = region + 1 - 2 * lax.rem(region, 2)

    core = lax.rem(region, 2)
    spot = region // 2
    spots = patches // 2
    near, far = split_peers(groups)
    rounds = hub_sem.shape[0]
    barrier = pltpu.get_barrier_semaphore()
    for r in near:
        hub = {"member": member_peer(me, r, groups), "grid": 2 * spot + 1}
        pl.semaphore_signal(barrier, inc=1, device_id=hub, device_id_type=MESH)

    @pl.when(core == 0)
    def _():
        pl.semaphore_signal(barrier, inc=1, device_id={"grid": partner}, device_id_type=MESH)

    def tell_hubs(t):
        for r in near:
            hub = {"member": member_peer(me, r, groups)}
            pl.semaphore_signal(hub_sem.at[t], inc=1, device_id=hub, device_id_type=MESH)

    def meet_near():
        @pl.when(core == 1)
        def _():
            pl.semaphore_wait(barrier, 2 * len(near) + 1)
            pl.semaphore_signal(near_sem, inc=1, device_id={"grid": partner}, device_id_type=MESH)
            if far:
                tell_hubs(0)

        @pl.when(core == 0)
        def _():
            pl.semaphore_wait(near_sem, 1)
            for d in range(1, spots):
                other = 2 * lax.rem(spot + d, spots)
                pl.semaphore_signal(barrier, inc=1, device_id={"grid": other}, device_id_type=MESH)

    def meet_all():
        @pl.when(core == 1)
        def _():
            for t in range(rounds):
                pl.semaphore_wait(hub_sem.at[t], len(near))
                if t + 1 < rounds:
                    tell_hubs(t + 1)
            pl.semaphore_signal(all_sem, inc=1, device_id={"grid": partner}, device_id_type=MESH)

        @pl.when(core == 0)
        def _():
            pl.semaphore_wait(all_sem, 1)

    def meet_grid():
        @pl.when(core == 0)
        def _():
            pl.semaphore_wait(barrier, spots - 1)
            pl.semaphore_signal(far_sem, inc=1, device_id={"grid": partner}, device_id_type=MESH)

        @pl.when(core == 1)
        def _():
            pl.semaphore_wait(far_sem, 1)

    def forecast(c, r, staged=0):
        peer = member_peer(me, r, groups)
        at = pl.ds(pl.multiple_of(peer * columns + c * width, width), width)
        if staged == 1:
            at = pl.ds(pl.multiple_of(peer * columns + LANES, LANES), width - LANES)
        source = stage_ref.at[r - 1] if staged == 2 else prior_hbm.at[:, :, at]
        target = x_ref.at[c, me]
        if staged:
            target = target.at[:, :, LANES:] if staged == 1 else target.at[:, :, 0:LANES]
        return pltpu.make_async_remote_copy(
            src_ref=source,
            dst_ref=target,
            send_sem=xs_sem,
            recv_sem=xr_sem.at[c],
            device_id={"member": peer},
            device_id_type=MESH,
        )

    def send_forecasts(first, last):
        def some(c, carry):
            for r in range(1, groups):
                forecast(c, r).start()
            return carry

        lax.fori_loop(first, last, some, 0)

    def arrived(ref, sem):
        pltpu.make_async_copy(ref, ref, sem).wait()

    early = (chunks + 1) // 2
    for r in range(1, groups):
        at = pl.ds(pl.multiple_of(member_peer(me, r, groups) * columns, LANES), LANES)
        pltpu.make_async_copy(prior_hbm.at[:, :, at], stage_ref.at[r - 1], stage_sem).start()
    local = [
        pltpu.make_async_copy(triples_hbm.at[:, 0], triples_ref, local_sem.at[0]),
        pltpu.make_async_copy(factors_hbm.at[:, 0], factors_ref, local_sem.at[1]),
        pltpu.make_async_copy(transforms_hbm, t32_ref, local_sem.at[2]),
        pltpu.make_async_copy(mapping_hbm, mapping_ref, local_sem.at[3]),
    ]
    for copy in local:
        copy.start()
    meet_near()
    arrived(stage_ref, stage_sem)
    for staged in (2, 1):
        for r in near:
            forecast(0, r, staged).start()
    if far:
        meet_all()
    for staged in (2, 1):
        for r in far:
            forecast(0, r, staged).start()
    send_forecasts(1, early)

    def own_forecast(c, carry):
        at = pl.ds(pl.multiple_of(me * columns + c * width, width), width)
        pltpu.make_async_copy(prior_hbm.at[:, :, at], x_ref.at[c, me], xr_sem.at[c]).start()
        return carry

    lax.fori_loop(0, chunks, own_forecast, 0)

    local[0].wait()
    local[1].wait()
    raw = factors_ref[...]
    shares = raw / jnp.sum(raw, axis=0, keepdims=True)
    points = triples_ref[...].astype(jnp.float32) + 1.0
    blank = jnp.zeros((2, per_source), jnp.float32)
    if per_source < LANES:
        meta_out_ref[...] = jnp.zeros_like(meta_out_ref)
    for h in range(patches):
        part = slice(h * per_source, (h + 1) * per_source)
        meta_out_ref[h, :, 0:per_source] = jnp.concatenate(
            [points[:, part], shares[:, part], blank], axis=0
        )

    def table(d):
        peer = lax.rem(region + d, patches)
        return pltpu.make_async_remote_copy(
            src_ref=meta_out_ref.at[peer],
            dst_ref=meta_in_ref.at[region],
            send_sem=ms_sem,
            recv_sem=mr_sem,
            device_id={"grid": peer},
            device_id_type=MESH,
        )

    local[2].wait()

    def block_of(q, part):
        rows = pairs // HALVES
        lanes = pl.ds(pl.multiple_of(q * coarse_dev, coarse_dev), coarse_dev)
        return tall_ref.at[part * rows : (part + 1) * rows, lanes]

    rows = pairs // 10

    def narrow(i, carry):
        at = pl.ds(pl.multiple_of(i * rows, rows), rows)
        lanes = pl.ds(pl.multiple_of(region * coarse_dev, coarse_dev), coarse_dev)
        tall_ref[at, lanes] = t32_ref[at, :].astype(jnp.bfloat16)
        return carry

    lax.fori_loop(0, 10, narrow, 0)
    def along(way, s, part):
        block = block_of(region - 2 * way * s, part)
        return pltpu.make_async_remote_copy(
            src_ref=block,
            dst_ref=block,
            send_sem=ts_sem.at[(1 + way) // 2],
            recv_sem=tr_sem.at[(1 + way) // 2, s, part],
            device_id={"grid": region + 2 * way},
            device_id_type=MESH,
        )

    def across(at, part):
        block = block_of(2 * at + core, part)
        return pltpu.make_async_remote_copy(
            src_ref=block,
            dst_ref=block,
            send_sem=fs_sem,
            recv_sem=fr_sem,
            device_id={"grid": partner},
            device_id_type=MESH,
        )

    def has_next(way):
        return spot + 1 < spots if way == 1 else spot > 0

    def has_source(way, s):
        return spot >= s if way == 1 else spot + s < spots

    def relay(s, part):
        for way in (1, -1):

            @pl.when(has_source(way, s))
            def _(way=way):
                along(way, s - 1, part).wait_recv()

                @pl.when(has_next(way))
                def _():
                    along(way, s, part).start()

                across(spot - way * s, part).start()

    meet_grid()
    for d in range(1, patches):
        table(d).start()
    meta_in_ref[region] = meta_out_ref[region]

    for way in (1, -1):

        @pl.when(has_next(way))
        def _(way=way):
            for part in range(HALVES):
                along(way, 0, part).start()

    for part in range(HALVES):
        across(spot, part).start()

    arrived(meta_in_ref.at[1:], mr_sem)
    for first in range(0, patches, 8):
        packed = jnp.concatenate([meta_in_ref[first + u, 0:6] for u in range(8)], axis=0)
        meta_ref[me, first // 8] = packed.astype(jnp.bfloat16)

    def tables(r):
        return pltpu.make_async_remote_copy(
            src_ref=meta_ref.at[me],
            dst_ref=meta_ref.at[me],
            send_sem=ns_sem,
            recv_sem=nr_sem,
            device_id={"member": member_peer(me, r, groups)},
            device_id_type=MESH,
        )

    for r in range(1, groups):
        tables(r).start()
    send_forecasts(early, chunks)

    def arrive(c):
        arrived(x_ref.at[c], xr_sem.at[c])

    def center(c):
        for lane in range(0, width, LANES):
            lanes = slice(lane, lane + LANES)

            def add(kk, total, lanes=lanes):
                for g in range(groups):
                    total = total + x_ref[c, g, kk, :, lanes].astype(jnp.float32)
                return total

            total = lax.fori_loop(0, mine, add, jnp.zeros((fields, LANES), jnp.float32))
            mean = total / members
            mean_ref[c, :, lanes] = mean

            def less(kk, carry, lanes=lanes, mean=mean):
                for g in range(groups):
                    d = x_ref[c, g, kk, :, lanes].astype(jnp.float32) - mean
                    dev_ref[c, g * mine + kk, :, lanes] = d.astype(jnp.bfloat16).astype(jnp.float32)
                return carry

            lax.fori_loop(0, mine, less, 0)

    def early_center(c, carry):
        arrive(c)
        center(c)
        return carry

    hops = [(s, part) for s in range(1, spots) for part in range(HALVES)]
    middle = HALVES * ((spots + 1) // 2)
    for hop in hops[:1]:
        relay(*hop)
    early_center(0, 0)
    for hop in hops[1:middle]:
        relay(*hop)
    lax.fori_loop(1, early, early_center, 0)

    local[3].wait()
    arrived(meta_ref.at[1:], nr_sem)
    cells = lax.broadcasted_iota(jnp.int32, (columns, per_source), 0) + me * columns

    def look(octet, found):
        ids, shares = found
        for m in range(groups):
            packed = meta_ref[m, octet]
            if per_source < LANES:
                packed = packed[:, 0:per_source]
            for u in range(8):
                source = 8 * octet + u
                onehot = jnp.where(cells == mapping_ref[source, m : m + 1, :], 1.0, 0.0)
                hit = lax.dot_general(
                    packed,
                    onehot.astype(jnp.bfloat16),
                    (((1,), (1,)), ((), ())),
                    preferred_element_type=jnp.float32,
                )[6 * u : 6 * u + 6]
                base = (jnp.int32(source * coarse_dev) - (RIM + 1)).astype(jnp.float32)
                ids = ids + jnp.where(hit[0:1] > 0.5, hit[0:3] + base, 0.0)
                shares = shares + hit[3:6]
        return ids, shares

    nothing = jnp.zeros((3, columns), jnp.float32)
    ids, shares = lax.fori_loop(0, patches // 8, look, (nothing, nothing))
    ids = jnp.where(ids < 0.0, ids + coarse, ids)
    ids = jnp.where(ids >= coarse, ids - coarse, ids)
    for c in range(chunks):
        ids_ref[c, 0:3] = ids[:, c * width : (c + 1) * width]
        share_ref[c, 0:3] = shares[:, c * width : (c + 1) * width]

    for hop in hops[middle:]:
        relay(*hop)
    arrived(tall_ref.at[:, 0 : spots * coarse_dev], fr_sem)

    def result(b, r):
        peer = member_peer(me, r, groups)
        at = pl.ds(pl.multiple_of(me * columns + b * LANES, LANES), LANES)
        return pltpu.make_async_remote_copy(
            src_ref=result_ref.at[b, pl.ds(peer * mine, mine)],
            dst_ref=out_hbm.at[:, :, at],
            send_sem=os_sem,
            recv_sem=or_sem,
            device_id={"member": peer},
            device_id_type=MESH,
        )

    def own_result(b):
        at = pl.ds(pl.multiple_of(me * columns + b * LANES, LANES), LANES)

        def put(kk, carry):
            out_hbm[kk, :, at] = result_ref[b, me * mine + kk]
            return carry

        lax.fori_loop(0, mine, put, 0)

    step = pairs // 4
    unroll = 8

    def update(c, carry):
        @pl.when(c >= early)
        def _():
            arrive(c)
            center(c)

        def place(q, z):
            at = pl.multiple_of(q * coarse_dev, coarse_dev)
            slots = lax.broadcasted_iota(jnp.int32, (coarse_dev, width), 0) + at
            slots = slots.astype(jnp.float32)
            spread = jnp.zeros((coarse_dev, width), jnp.float32)
            for s in range(3):
                hit = ids_ref[c, s : s + 1, :] == slots
                spread = spread + jnp.where(hit, share_ref[c, s : s + 1, :], 0.0)
            spread_ref[pl.ds(at, coarse_dev), :] = spread.astype(jnp.bfloat16)
            return z

        lax.fori_loop(0, patches, place, 0)

        def blend(i, z):
            at = pl.ds(pl.multiple_of(i * step, step), step)
            part = jnp.dot(tall_ref[at, :], spread_ref[...], preferred_element_type=jnp.float32)
            w_ref[pl.ds(i * (step // 8), step // 8)] = part.reshape(step // 8, 8, width)
            return z

        lax.fori_loop(0, 4, blend, 0)

        for lane in range(0, width, LANES):
            lanes = slice(lane, lane + LANES)
            b = c * (width // LANES) + lane // LANES

            def contract(jg, z, lanes=lanes, b=b):
                for first in (0, 4):

                    def some(kk, accs, first=first):
                        accs = list(accs)
                        for u in range(unroll):
                            k = kk * unroll + u
                            d = dev_ref[c, k, :, lanes]
                            for jj in range(4):
                                row = first + jj
                                w = w_ref[k * (members // 8) + jg, row : row + 1, lanes]
                                accs[jj] = accs[jj] + d * w
                        return tuple(accs)

                    start = tuple(mean_ref[c, :, lanes] for _ in range(4))
                    accs = lax.fori_loop(0, members // unroll, some, start)
                    for jj in range(4):
                        result_ref[b, jg * 8 + first + jj] = accs[jj].astype(jnp.bfloat16)
                return z

            lax.fori_loop(0, members // 8, contract, 0)
            for r in range(1, groups):
                result(b, r).start()
            own_result(b)
        return carry

    lax.fori_loop(0, chunks, update, 0)

    arrived(meta_in_ref.at[1:], ms_sem)
    arrived(meta_ref.at[1:], ns_sem)
    for n in range(1, spots):
        for side, mark in ((1, n - 1), (0, spots - n)):

            @pl.when(spot == mark)
            def _(n=n, side=side):
                arrived(tall_ref.at[:, 0 : n * coarse_dev], ts_sem.at[side])

    arrived(tall_ref.at[:, 0 : spots * coarse_dev], fs_sem)
    others = x_ref.at[:, 1:]
    arrived(others, xs_sem)
    arrived(others, os_sem)
    arrived(others, or_sem)


def on_device(prior, mapping, triples, factors, transforms):
    groups = lax.axis_size("member")
    patches = lax.axis_size("grid")
    mine, fields, cells = prior.shape
    members = mine * groups
    columns = cells // groups
    per_source = mapping.shape[2]
    pairs, coarse_dev = transforms.shape
    coarse = coarse_dev * patches
    width = min(256, columns)
    chunks = columns // width
    blocks = columns // LANES
    anywhere = pl.BlockSpec(memory_space=pl.ANY)
    dma = pltpu.SemaphoreType.DMA
    return pl.pallas_call(
        functools.partial(exchange_kernel, groups, patches),
        out_shape=pltpu.VMEM(prior.shape, jnp.bfloat16),
        in_specs=[anywhere] * 5,
        out_specs=pl.BlockSpec(memory_space=pltpu.VMEM),
        scratch_shapes=[
            pltpu.VMEM((patches, groups, per_source), jnp.int32),
            pltpu.VMEM((3, columns), jnp.int32),
            pltpu.VMEM((3, columns), jnp.float32),
            pltpu.VMEM((pairs, coarse_dev), jnp.float32),
            pltpu.VMEM((pairs, coarse), jnp.bfloat16),
            pltpu.VMEM((patches, 8, LANES), jnp.float32),
            pltpu.VMEM((patches, 8, LANES), jnp.float32),
            pltpu.VMEM((groups, patches // 8, 48, LANES), jnp.bfloat16),
            pltpu.VMEM((chunks, 8, width), jnp.float32),
            pltpu.VMEM((chunks, 8, width), jnp.float32),
            pltpu.VMEM((chunks, groups, mine, fields, width), jnp.bfloat16),
            pltpu.VMEM((chunks, members, fields, width), jnp.float32),
            pltpu.VMEM((chunks, fields, width), jnp.float32),
            pltpu.VMEM((coarse, width), jnp.bfloat16),
            pltpu.VMEM((pairs // 8, 8, width), jnp.float32),
            pltpu.VMEM((blocks, members, fields, LANES), jnp.bfloat16),
            pltpu.VMEM((groups - 1, mine, fields, LANES), jnp.bfloat16),
            dma((4,)),
            dma,
            dma,
            dma((chunks,)),
            pltpu.SemaphoreType.REGULAR,
            pltpu.SemaphoreType.REGULAR,
            pltpu.SemaphoreType.REGULAR,
            pltpu.SemaphoreType.REGULAR((max(groups.bit_length() - 2, 1),)),
            dma((2,)),
            dma((2, patches // 2 - 1, HALVES)),
            dma,
            dma,
            dma,
            dma,
            dma,
            dma,
            dma,
            dma,
        ],
        compiler_params=pltpu.CompilerParams(
            collective_id=0, has_side_effects=True, vmem_limit_bytes=44 * 1024 * 1024
        ),
        name="exchange",
    )(*[
        pltpu.with_memory_space_constraint(a, pltpu.HBM)
        for a in (
            mapping,
            jnp.transpose(triples, (1, 0, 2)),
            jnp.transpose(factors, (1, 0, 2)),
            transforms,
            prior,
        )
    ])


def solution(mesh):
    return jax.shard_map(
        on_device,
        mesh=mesh,
        in_specs=(
            P("member", None, "grid"),
            P(None, None, "grid"),
            P("grid", None, "member"),
            P("grid", None, "member"),
            P(None, "grid"),
        ),
        out_specs=P("member", None, "grid"),
        check_vma=False,
    )
```
